512 devices in a mesh: body: 2 (over y), gx: 16 (over z), gy: 8 (over x), gz: 2 (over core).
Axes of the slice: x: 8, y: 2, z: 16, core: 2. Of those that a mesh axis runs over, the one named last changes fastest.
The devices are a block of a 8x8x16 slice.
Arguments:
- fields: float32 [4, 3, 64, 64, 256], P('body', None, 'gx', 'gy', 'gz'), parts along dimension 0, may hold values from -0.06 to 0.06
- macro_strain: float32 [6, 3], P('body'), parts along dimension 0, may hold values from -0.15 to 0.15
- material: float32 [4], P('body'), parts along dimension 0, may hold values from 2 to 10
Outputs:
- residual: float32 [6, 64, 64, 256], P('body', 'gx', 'gy', 'gz'), parts along dimension 0
- tangent: float32 [6, 64, 64, 256], P('body', 'gx', 'gy', 'gz'), parts along dimension 0
- stats: float32 [4], P('body'), parts along dimension 0
The draws below stay inside these ranges and needn't reach their ends.
There are 2 independent parts, one for each index of `body`. The reference program is written for one: setup_inputs(seed, part) draws one part's arguments, and reference() takes and returns one part's arrays. A program takes and returns all parts, laid end to end along the dimension named above; each array names one. Nothing has to cross between parts.
All inputs are finite; a program needn't handle non-finite values.
Results may differ from the reference program's by a relative error of at most 0.0002.
Values sent between devices are 32-bit elements; how exact they have to be, the bound alone decides.
A program may use at most 64 MiB of HBM per device.

```python
import math
import jax
import jax.numpy as jnp
import numpy as np
from jax import lax

NEX = 32
NX = 64
NY = 64
NZ = 256


def draw_fields(key, part):
    bound_value = 0.06
    full_shape = (2, 3, NX, NY, NZ)
    noise_draw = jax.random.uniform(key, full_shape, jnp.float32, -1.0, 1.0)
    rising = (1.0 + 2.0 * jnp.arange(NX, dtype=jnp.float32) / (NX - 1)) / 3.0
    rising = rising[:, None, None]
    combined = noise_draw
    return (bound_value * rising * combined).astype(jnp.float32)


def setup_inputs(seed: int = 0, part: int = 0) -> dict:
    streams_of = jax.random.split(jax.random.key(seed), 4)
    part_keys = jax.random.split(jax.random.fold_in(streams_of[3], part), 4)
    fields = draw_fields(jax.random.fold_in(jax.random.fold_in(streams_of[3], part), 71), part)
    macro_strain = jnp.clip(jax.random.uniform(part_keys[1], (3, 3), jnp.float32, -0.15, 0.15), -0.15, 0.15)
    material = jnp.clip(jnp.exp(jax.random.uniform(part_keys[2], (2,), jnp.float32, math.log(2.0), math.log(10.0))), 2.0, 10.0)
    return dict(fields=fields, macro_strain=macro_strain, material=material)


highest = lax.Precision.HIGHEST
spacing = 4.0
root_eps = 1e-06

def shape_tables():
    gauss_root = math.sqrt(0.6)
    points = np.array([-gauss_root, 0.0, gauss_root])
    values = np.stack([points * (points - 1.0) / 2.0, 1.0 - points * points, points * (points + 1.0) / 2.0], axis=1)
    slopes = np.stack([points - 0.5, -2.0 * points, points + 0.5], axis=1) * (2.0 / spacing)
    weights = np.array([5.0 / 9.0, 8.0 / 9.0, 5.0 / 9.0])
    volume = weights[:, None, None] * weights[None, :, None] * weights[None, None, :] * (spacing / 2.0) ** 3
    return (jnp.asarray(values, jnp.float32), jnp.asarray(slopes, jnp.float32), jnp.asarray(volume, jnp.float32))

def triplets(array, axis, periodic):
    length = array.shape[axis]
    if periodic:
        even_nodes = lax.slice_in_dim(array, 0, length, 2, axis)
        odd_nodes = lax.slice_in_dim(array, 1, length, 2, axis)
        next_nodes = jnp.roll(even_nodes, -1, axis)
    else:
        elements = (length - 1) // 2
        even_nodes = lax.slice_in_dim(array, 0, 2 * elements, 2, axis)
        odd_nodes = lax.slice_in_dim(array, 1, 2 * elements, 2, axis)
        next_nodes = lax.slice_in_dim(array, 2, 2 * elements + 1, 2, axis)
    return jnp.stack([even_nodes, odd_nodes, next_nodes], axis=2)

def scatter_back(stacked, periodic):
    pieces = [lax.index_in_dim(stacked, slot_index, 2, keepdims=False) for slot_index in range(3)]
    if periodic:
        even_nodes = pieces[0] + jnp.roll(pieces[2], 1, axis=3)
        odd_nodes = pieces[1]
    else:
        pad_after = [(0, 0)] * pieces[0].ndim
        pad_after[3] = (0, 1)
        pad_before = [(0, 0)] * pieces[0].ndim
        pad_before[3] = (1, 0)
        even_nodes = jnp.pad(pieces[0], pad_after) + jnp.pad(pieces[2], pad_before)
        odd_nodes = jnp.pad(pieces[1], pad_after)
    paired = jnp.stack([even_nodes, odd_nodes], axis=4)
    merged_shape = paired.shape[:3] + (2 * paired.shape[3],) + paired.shape[5:]
    merged = paired.reshape(merged_shape)
    if not periodic:
        merged = lax.slice_in_dim(merged, 0, merged.shape[3] - 1, 1, 3)
    return merged

def stresses(grads, strain, shear, lame_first):
    deform = [[grads[col_at][row_at] + strain[row_at, col_at] + (1.0 if row_at == col_at else 0.0) for col_at in range(3)] for row_at in range(3)]
    change = [[grads[col_at][3 + row_at] for col_at in range(3)] for row_at in range(3)]
    cofactor = [[deform[(row_at + 1) % 3][(col_at + 1) % 3] * deform[(row_at + 2) % 3][(col_at + 2) % 3] - deform[(row_at + 1) % 3][(col_at + 2) % 3] * deform[(row_at + 2) % 3][(col_at + 1) % 3] for col_at in range(3)] for row_at in range(3)]
    volume_ratio = deform[0][0] * cofactor[0][0] + deform[0][1] * cofactor[0][1] + deform[0][2] * cofactor[0][2]
    inverse_t = [[cofactor[row_at][col_at] / volume_ratio for col_at in range(3)] for row_at in range(3)]
    log_ratio = jnp.log(volume_ratio)
    stress = [[shear * (deform[row_at][col_at] - inverse_t[row_at][col_at]) + lame_first * log_ratio * inverse_t[row_at][col_at] for col_at in range(3)] for row_at in range(3)]
    trace_term = sum((inverse_t[row_at][col_at] * change[row_at][col_at] for row_at in range(3) for col_at in range(3)))
    product = [[sum((inverse_t[row_at][mid_at] * change[col_at][mid_at] for mid_at in range(3))) for col_at in range(3)] for row_at in range(3)]
    twisted = [[sum((product[row_at][mid_at] * inverse_t[mid_at][col_at] for mid_at in range(3))) for col_at in range(3)] for row_at in range(3)]
    softening = shear - lame_first * log_ratio
    dstress = [[shear * change[row_at][col_at] + softening * twisted[row_at][col_at] + lame_first * trace_term * inverse_t[row_at][col_at] for col_at in range(3)] for row_at in range(3)]
    return (stress, dstress)

def layer_forces(slab_nodes, strain, material, periodic):
    values, slopes, volume = shape_tables()
    stacked = triplets(triplets(slab_nodes, 3, periodic), 3, periodic)
    z_value = jnp.einsum('qa,cxyaij->cxyqij', values, stacked, precision=highest)
    z_slope = jnp.einsum('qa,cxyaij->cxyqij', slopes, stacked, precision=highest)
    y_value = jnp.einsum('qa,cxazij->cxqzij', values, z_value, precision=highest)
    y_slope = jnp.einsum('qa,cxazij->cxqzij', slopes, z_value, precision=highest)
    yz_slope = jnp.einsum('qa,cxazij->cxqzij', values, z_slope, precision=highest)
    grads = [jnp.einsum('qa,cayzij->cqyzij', slopes, y_value, precision=highest), jnp.einsum('qa,cayzij->cqyzij', values, y_slope, precision=highest), jnp.einsum('qa,cayzij->cqyzij', values, yz_slope, precision=highest)]
    stress, dstress = stresses(grads, strain, material[0], material[1])
    weight = volume[:, :, :, None, None]
    fluxes = [jnp.stack([stress[0][along], stress[1][along], stress[2][along], dstress[0][along], dstress[1][along], dstress[2][along]]) * weight for along in range(3)]
    back_x0 = jnp.einsum('qa,cqyzij->cayzij', slopes, fluxes[0], precision=highest)
    back_x1 = jnp.einsum('qa,cqyzij->cayzij', values, fluxes[1], precision=highest)
    back_x2 = jnp.einsum('qa,cqyzij->cayzij', values, fluxes[2], precision=highest)
    back_y = jnp.einsum('qa,cxqzij->cxazij', values, back_x0, precision=highest) + jnp.einsum('qa,cxqzij->cxazij', slopes, back_x1, precision=highest)
    back_yz = jnp.einsum('qa,cxqzij->cxazij', values, back_x2, precision=highest)
    back_z = jnp.einsum('qa,cxyqij->cxyaij', values, back_y, precision=highest) + jnp.einsum('qa,cxyqij->cxyaij', slopes, back_yz, precision=highest)
    return scatter_back(scatter_back(back_z, periodic), periodic)

def reference(fields, macro_strain, material):
    flat = fields.reshape((6, NX, NY, NZ))
    closed = jnp.concatenate([flat, flat[:, :1]], axis=1)

    def one_layer(layer_index, accumulated):
        plane_start = (2 * layer_index).astype(jnp.int32)
        slab_nodes = lax.dynamic_slice_in_dim(closed, plane_start, 3, 1)
        contribution = layer_forces(slab_nodes, macro_strain, material, True)
        current = lax.dynamic_slice_in_dim(accumulated, plane_start, 3, 1)
        return lax.dynamic_update_slice_in_dim(accumulated, current + contribution, plane_start, 1)
    accumulated = lax.fori_loop(0, NEX, one_layer, jnp.zeros(closed.shape, jnp.float32))
    folded = jnp.concatenate([accumulated[:, :1] + accumulated[:, NX:], accumulated[:, 1:NX]], axis=1)
    residual = folded[:3]
    tangent = folded[3:]
    entries = 3.0 * NX * NY * NZ
    squares = jnp.sum(residual * residual)
    curvature = jnp.sum(flat[3:] * tangent)
    stats = jnp.stack([jnp.sqrt(squares / entries + root_eps), curvature / entries])
    return (residual, tangent, stats)
```

```python
import functools
import math

import jax
import jax.numpy as jnp
import numpy as np
from jax import lax
from jax.experimental import pallas as pl
from jax.experimental.pallas import tpu as pltpu
from jax.sharding import PartitionSpec as P

MESH = pl.DeviceIdType.MESH
spacing = 4.0
root_eps = 1e-06
f32 = jnp.float32
bf16 = jnp.bfloat16


def tables():
    root = math.sqrt(0.6)
    points = np.array([-root, 0.0, root])
    values = np.stack(
        [points * (points - 1.0) / 2.0, 1.0 - points * points, points * (points + 1.0) / 2.0], axis=1
    )
    slopes = np.stack([points - 0.5, -2.0 * points, points + 0.5], axis=1) * (2.0 / spacing)
    weights = np.array([5.0 / 9.0, 8.0 / 9.0, 5.0 / 9.0]) * (spacing / 2.0)
    return values, slopes, weights


def ceil_to(n, m):
    return -(-n // m) * m


class Layout:
    def __init__(self, nx, ny, nz):
        self.nx, self.ny, self.nz = nx, ny, nz
        self.own = nx * ny
        self.xm = self.own
        self.xp = self.xm + 2 * ny
        self.ym_own = self.xp + ny
        self.ym_xm = self.ym_own + 2 * nx
        self.ym_xp = self.ym_xm + 4
        self.yp_own = self.ym_xp + 2
        self.yp_xm = self.yp_own + nx
        self.yp_xp = self.yp_xm + 2
        self.used = self.yp_xp + 1
        self.rows = ceil_to(self.used, 16)
        self.ex, self.ey, self.ez = nx // 2 + 1, ny // 2 + 1, nz // 2 + 1
        self.group = ceil_to(self.ex * self.ey, 16)
        self.points = 9 * self.group
        self.lanes = ceil_to(3 * self.ez, 128)

    def row(self, p, r):
        if 0 <= r < self.ny:
            if 0 <= p < self.nx:
                return p * self.ny + r
            if p < 0:
                return self.xm + (p + 2) * self.ny + r
            return self.xp + r
        if r < 0:
            if 0 <= p < self.nx:
                return self.ym_own + 2 * p + r + 2
            if p < 0:
                return self.ym_xm + 2 * (p + 2) + r + 2
            return self.ym_xp + r + 2
        if 0 <= p < self.nx:
            return self.yp_own + p
        if p < 0:
            return self.yp_xm + p + 2
        return self.yp_xp


def split_np(a):
    a = a.astype(np.float32)
    high = np.asarray(a, dtype=jnp.bfloat16)
    low = np.asarray(a - high.astype(np.float32), dtype=jnp.bfloat16)
    return high, low


def matrices(lay):
    values, slopes, weights = tables()
    forward = np.zeros((3, lay.points, lay.rows))
    back = np.zeros((3, lay.own, lay.points))
    pairs = ((slopes, values), (values, slopes), (values, values))
    for kind, (tx, ty) in enumerate(pairs):
        for q1 in range(3):
            for q2 in range(3):
                for ex in range(lay.ex):
                    for ey in range(lay.ey):
                        point = (q1 * 3 + q2) * lay.group + ex * lay.ey + ey
                        for a1 in range(3):
                            for a2 in range(3):
                                p, r = 2 * (ex - 1) + a1, 2 * (ey - 1) + a2
                                factor = tx[q1, a1] * ty[q2, a2]
                                forward[kind, point, lay.row(p, r)] += factor
                                if 0 <= p < lay.nx and 0 <= r < lay.ny:
                                    back[kind, p * lay.ny + r, point] += factor * weights[q1] * weights[q2]
    along_z = np.zeros((2, 2 * lay.nz, lay.lanes))
    z_back = np.zeros((2, lay.lanes, lay.nz))
    for kind, tz in enumerate((values, slopes)):
        for q3 in range(3):
            for ez in range(lay.ez):
                for a3 in range(3):
                    z = 2 * (ez - 1) + a3
                    column = q3 * lay.ez + ez
                    if z < 0:
                        k = lay.nz + lay.nz + z
                    elif z >= lay.nz:
                        k = lay.nz + z - lay.nz
                    else:
                        k = z
                        z_back[kind, column, z] += tz[q3, a3] * weights[q3]
                    along_z[kind, k, column] += tz[q3, a3]
    along_z = np.concatenate([along_z[0], along_z[1]], axis=1)
    fh, fl = split_np(forward)
    forward = np.concatenate([fh, fh, fl], axis=2)
    bh, bl = split_np(back)
    back = np.concatenate([bh, bl], axis=1)
    along_z = np.stack(split_np(along_z))
    z_back = np.stack(split_np(z_back), axis=1)
    return forward, back, along_z, z_back


def split(x):
    high = x.astype(bf16)
    return high, (x - high.astype(f32)).astype(bf16)


def dot(a, b):
    return jnp.dot(a, b, preferred_element_type=f32)


def kernel(
    lay, sizes,
    fields, strain, material, forward_h, back_h, along_h, z_back_h,
    residual_h, tangent_h, stats,
    ext, extp, forward, back, along, z_back, grads, flux, out, send_a, recv_a, send_b, recv_b,
    load_sem, const_sem, halo_send, halo_recv, core_send, core_recv, out_sem,
    a_send, a_recv, b_send, b_recv, far_sem,
):
    n = dict(sizes)
    me = {axis: lax.axis_index(axis) for axis in ("gx", "gy", "gz")}
    nx, ny, nz = lay.nx, lay.ny, lay.nz

    def device(**shifts):
        return {
            axis: lax.rem(me[axis] + (shift % n[axis]), n[axis]) for axis, shift in shifts.items()
        }

    load = pltpu.make_async_copy(fields, ext.at[:, 0 : lay.own, :], load_sem)
    load.start()

    barrier = pltpu.get_barrier_semaphore()
    near = (device(gz=1), device(gx=1), device(gx=-1), device(gy=1), device(gy=-1))
    for where in near:
        pl.semaphore_signal(barrier, inc=1, device_id=where, device_id_type=MESH)

    constants = [
        pltpu.make_async_copy(source, target, const_sem.at[i])
        for i, (source, target) in enumerate(
            ((along_h, along), (forward_h, forward), (back_h, back), (z_back_h, z_back))
        )
    ]
    for copy in constants:
        copy.start()
    tail = lay.rows - lay.used
    if tail:
        ext[:, lay.used :, :] = jnp.zeros((6, tail, nz), f32)

    count = [0]
    sends = []

    def send(source, target, where):
        i = count[0]
        count[0] += 1
        copy = pltpu.make_async_remote_copy(
            src_ref=ext.at[:, source[0] : source[0] + source[1], :],
            dst_ref=ext.at[:, target : target + source[1], :],
            send_sem=halo_send.at[i],
            recv_sem=halo_recv.at[i],
            device_id=where,
            device_id_type=MESH,
        )
        copy.start()
        sends.append(copy)

    load.wait()
    pl.semaphore_wait(barrier, len(near))
    send(((nx - 2) * ny, 2 * ny), lay.xm, device(gx=1))
    send((0, ny), lay.xp, device(gx=-1))
    for p in range(nx):
        send((p * ny + ny - 2, 2), lay.ym_own + 2 * p, device(gy=1))
        send((p * ny, 1), lay.yp_own + p, device(gy=-1))
    to_core = device(gz=1)
    core_own = pltpu.make_async_remote_copy(
        src_ref=ext.at[:, 0 : lay.own, :],
        dst_ref=extp.at[:, 0 : lay.own, :],
        send_sem=core_send.at[0],
        recv_sem=core_recv.at[0],
        device_id=to_core,
        device_id_type=MESH,
    )
    core_own.start()

    def greet(step):
        d = 2**step
        for where in (device(gx=d), device(gx=-d), device(gy=d), device(gy=-d)):
            pl.semaphore_signal(far_sem.at[step], inc=1, device_id=where, device_id_type=MESH)

    rounds = 1
    while 2**rounds < n["gx"] // 2 or 2**rounds <= n["gy"] // 2:
        rounds += 1
    greet(0)
    pl.semaphore_wait(far_sem.at[0], 4)
    for p in range(2):
        send(((nx - 2 + p) * ny + ny - 2, 2), lay.ym_xm + 2 * p, device(gx=1, gy=1))
        send(((nx - 2 + p) * ny, 1), lay.yp_xm + p, device(gx=1, gy=-1))
    send((ny - 2, 2), lay.ym_xp, device(gx=-1, gy=1))
    send((0, 1), lay.yp_xp, device(gx=-1, gy=-1))
    for step in range(1, rounds):
        greet(step)
        if step < rounds - 1:
            pl.semaphore_wait(far_sem.at[step], 4)

    for copy in sends:
        copy.wait()
    core_halo = pltpu.make_async_remote_copy(
        src_ref=ext.at[:, lay.own :, :],
        dst_ref=extp.at[:, lay.own :, :],
        send_sem=core_send.at[1],
        recv_sem=core_recv.at[1],
        device_id=to_core,
        device_id_type=MESH,
    )
    core_halo.start()
    for copy in constants:
        copy.wait()
    core_own.wait()
    core_halo.wait()

    lanes = lay.lanes
    for c in range(6):
        nodes = jnp.concatenate([ext[c], extp[c]], axis=1)
        high, low = split(nodes)
        z = dot(high, along[0]) + dot(low, along[0]) + dot(high, along[1])
        vh, vl = split(z[:, :lanes])
        sh, sl = split(z[:, lanes:])
        value = jnp.concatenate([vh, vl, vh], axis=0)
        slope = jnp.concatenate([sh, sl, sh], axis=0)
        grads[c, 0] = dot(forward[0], value)
        grads[c, 1] = dot(forward[1], value)
        grads[c, 2] = dot(forward[2], slope)

    shear, lame = material[0], material[1]
    ratio = lame / shear
    shift = [
        [strain[i, j] + (1.0 if i == j else 0.0) for j in range(3)] for i in range(3)
    ]

    def points(i, carry):
        for half in range(lanes // 128):
            at = (pl.ds(pl.multiple_of(i * 8, 8), 8), pl.ds(half * 128, 128))
            f = [[grads[(r, c) + at] + shift[r][c] for c in range(3)] for r in range(3)]
            dv = [[grads[(3 + r, c) + at] for c in range(3)] for r in range(3)]
            cof = [
                [
                    f[(r + 1) % 3][(c + 1) % 3] * f[(r + 2) % 3][(c + 2) % 3]
                    - f[(r + 1) % 3][(c + 2) % 3] * f[(r + 2) % 3][(c + 1) % 3]
                    for c in range(3)
                ]
                for r in range(3)
            ]
            det = f[0][0] * cof[0][0] + f[0][1] * cof[0][1] + f[0][2] * cof[0][2]
            inverse = 1.0 / det
            g = [[cof[r][c] * inverse for c in range(3)] for r in range(3)]
            pressure = ratio * jnp.log(det) - 1.0
            for r in range(3):
                for c in range(3):
                    flux[(r, c) + at] = f[r][c] + pressure * g[r][c]
            m = [
                [g[r][0] * dv[c][0] + g[r][1] * dv[c][1] + g[r][2] * dv[c][2] for c in range(3)]
                for r in range(3)
            ]
            trace = ratio * (m[0][0] + m[1][1] + m[2][2])
            w = [
                [trace - pressure * m[r][c] if r == c else -(pressure * m[r][c]) for c in range(3)]
                for r in range(3)
            ]
            for r in range(3):
                for c in range(3):
                    flux[(3 + r, c) + at] = dv[r][c] + (
                        w[r][0] * g[0][c] + w[r][1] * g[1][c] + w[r][2] * g[2][c]
                    )
        return carry

    lax.fori_loop(0, lay.points // 8, points, 0)

    own = lay.own
    squares = jnp.zeros((8, nz), f32)
    curvature = jnp.zeros((8, nz), f32)
    for c in range(6):
        def plane(kind, along_axis):
            high, low = split(flux[c, along_axis])
            both = dot(back[kind], high)
            return both[:own] + both[own:] + dot(back[kind, :own], low)

        vh, vl = split(plane(0, 0) + plane(1, 1))
        sh, sl = split(plane(2, 2))
        result = (
            dot(vh, z_back[0, 0]) + dot(vl, z_back[0, 0]) + dot(vh, z_back[0, 1])
            + dot(sh, z_back[1, 0]) + dot(sl, z_back[1, 0]) + dot(sh, z_back[1, 1])
        ) * shear
        out[c] = result
        product = result * result if c < 3 else result * ext[c, :own]
        part = product[0:8]
        for k in range(1, own // 8):
            part = part + product[8 * k : 8 * k + 8]
        if c < 3:
            squares = squares + part
        else:
            curvature = curvature + part

    writes = [
        pltpu.make_async_copy(out.at[0:3], residual_h, out_sem.at[0]),
        pltpu.make_async_copy(out.at[3:6], tangent_h, out_sem.at[1]),
    ]
    for copy in writes:
        copy.start()

    if rounds > 1:
        pl.semaphore_wait(far_sem.at[rounds - 1], 4)

    def exchange(totals, partners, sending, receiving, send_sems, recv_sems):
        sending[...] = totals
        copies = []
        for slot, where in enumerate(partners):
            copy = pltpu.make_async_remote_copy(
                src_ref=sending,
                dst_ref=receiving.at[slot],
                send_sem=send_sems.at[slot],
                recv_sem=recv_sems.at[slot],
                device_id=where,
                device_id_type=MESH,
            )
            copy.start()
            copies.append(copy)
        for copy in copies:
            copy.wait()
        return totals + jnp.sum(receiving[...], axis=0)

    totals = jnp.concatenate(
        [jnp.sum(squares, axis=0, keepdims=True), jnp.sum(curvature, axis=0, keepdims=True)], axis=0
    )
    half = n["gx"] // 2
    order = [k for d in range(half, 0, -1) for k in sorted({d, n["gx"] - d})]
    totals = exchange(
        totals, [device(gx=k) for k in order], send_a, recv_a, a_send, a_recv
    )
    half = n["gy"] // 2
    order = [k for d in range(half, 0, -1) for k in sorted({d, n["gy"] - d})] + [0]
    partners = []
    for k in order:
        partners.append(device(gy=k, gz=1))
        if k:
            partners.append(device(gy=k))
    totals = exchange(totals, partners, send_b, recv_b, b_send, b_recv)

    sums = jnp.sum(totals, axis=1, keepdims=True)
    entries = 3.0 * nx * ny * nz * n["gx"] * n["gy"] * n["gz"]
    means = sums / entries
    root = jnp.sqrt(means + root_eps)
    stats[0] = root[0, 0]
    stats[1] = means[1, 0]
    for copy in writes:
        copy.wait()


def solution(mesh):
    sizes = tuple((axis, mesh.shape[axis]) for axis in ("gx", "gy", "gz"))
    n = dict(sizes)

    def local(fields, macro_strain, material):
        nx, ny, nz = fields.shape[2:]
        lay = Layout(nx, ny, nz)
        consts = [jnp.asarray(m) for m in matrices(lay)]
        hbm = pl.BlockSpec(memory_space=pltpu.HBM)
        smem = pl.BlockSpec(memory_space=pltpu.SMEM)
        halos = 2 + 2 * nx + 6
        block = jax.ShapeDtypeStruct((3, lay.own, nz), f32)
        n_a, n_b = n["gx"] - 1, n["gy"] * n["gz"] - 1
        dma = pltpu.SemaphoreType.DMA
        residual, tangent, stats = pl.pallas_call(
            functools.partial(kernel, lay, sizes),
            out_shape=(block, block, jax.ShapeDtypeStruct((2,), f32)),
            in_specs=[hbm, smem, smem, hbm, hbm, hbm, hbm],
            out_specs=(hbm, hbm, smem),
            scratch_shapes=[
                pltpu.VMEM((6, lay.rows, nz), f32),
                pltpu.VMEM((6, lay.rows, nz), f32),
                *[pltpu.VMEM(m.shape, bf16) for m in consts],
                pltpu.VMEM((6, 3, lay.points, lay.lanes), f32),
                pltpu.VMEM((6, 3, lay.points, lay.lanes), f32),
                pltpu.VMEM((6, lay.own, nz), f32),
                pltpu.VMEM((2, nz), f32),
                pltpu.VMEM((n_a, 2, nz), f32),
                pltpu.VMEM((2, nz), f32),
                pltpu.VMEM((n_b, 2, nz), f32),
                dma,
                dma((4,)),
                dma((halos,)),
                dma((halos,)),
                dma((2,)),
                dma((2,)),
                dma((2,)),
                dma((n_a,)),
                dma((n_a,)),
                dma((n_b,)),
                dma((n_b,)),
                pltpu.SemaphoreType.REGULAR((8,)),
            ],
            compiler_params=pltpu.CompilerParams(collective_id=0, has_side_effects=True),
            name="cell",
        )(fields.reshape(6, nx * ny, nz), macro_strain, material, *consts)
        shape = (3, nx, ny, nz)
        return residual.reshape(shape), tangent.reshape(shape), stats

    in_specs = (P("body", None, "gx", "gy", "gz"), P("body", None), P("body"))
    out_specs = (P("body", "gx", "gy", "gz"), P("body", "gx", "gy", "gz"), P("body"))
    return jax.shard_map(local, mesh=mesh, in_specs=in_specs, out_specs=out_specs, check_vma=False)
```

```python
import functools
import math

import jax
import jax.numpy as jnp
import numpy as np
from jax import lax
from jax.experimental import pallas as pl
from jax.experimental.pallas import tpu as pltpu
from jax.sharding import PartitionSpec as P

MESH = pl.DeviceIdType.MESH
spacing = 4.0
root_eps = 1e-06
f32 = jnp.float32
bf16 = jnp.bfloat16


def tables():
    root = math.sqrt(0.6)
    points = np.array([-root, 0.0, root])
    values = np.stack(
        [points * (points - 1.0) / 2.0, 1.0 - points * points, points * (points + 1.0) / 2.0], axis=1
    )
    slopes = np.stack([points - 0.5, -2.0 * points, points + 0.5], axis=1) * (2.0 / spacing)
    weights = np.array([5.0 / 9.0, 8.0 / 9.0, 5.0 / 9.0]) * (spacing / 2.0)
    return values, slopes, weights


def ceil_to(n, m):
    return -(-n // m) * m


class Layout:
    def __init__(self, nx, ny, nz):
        self.nx, self.ny, self.nz = nx, ny, nz
        self.own = nx * ny
        self.xm = self.own
        self.xp = self.xm + 2 * ny
        self.ym_own = self.xp + ny
        self.ym_xm = self.ym_own + 2 * nx
        self.ym_xp = self.ym_xm + 4
        self.yp_own = self.ym_xp + 2
        self.yp_xm = self.yp_own + nx
        self.yp_xp = self.yp_xm + 2
        self.used = self.yp_xp + 1
        self.rows = ceil_to(self.used, 16)
        self.ex, self.ey, self.ez = nx // 2 + 1, ny // 2 + 1, nz // 2 + 1
        self.group = ceil_to(self.ex * self.ey, 16)
        self.points = 9 * self.group
        self.lanes = ceil_to(3 * self.ez, 128)

    def row(self, p, r):
        if 0 <= r < self.ny:
            if 0 <= p < self.nx:
                return p * self.ny + r
            if p < 0:
                return self.xm + (p + 2) * self.ny + r
            return self.xp + r
        if r < 0:
            if 0 <= p < self.nx:
                return self.ym_own + 2 * p + r + 2
            if p < 0:
                return self.ym_xm + 2 * (p + 2) + r + 2
            return self.ym_xp + r + 2
        if 0 <= p < self.nx:
            return self.yp_own + p
        if p < 0:
            return self.yp_xm + p + 2
        return self.yp_xp


def split_np(a):
    a = a.astype(np.float32)
    high = np.asarray(a, dtype=jnp.bfloat16)
    low = np.asarray(a - high.astype(np.float32), dtype=jnp.bfloat16)
    return high, low


def matrices(lay):
    values, slopes, weights = tables()
    forward = np.zeros((3, lay.points, lay.rows))
    back = np.zeros((3, lay.own, lay.points))
    pairs = ((slopes, values), (values, slopes), (values, values))
    for kind, (tx, ty) in enumerate(pairs):
        for q1 in range(3):
            for q2 in range(3):
                for ex in range(lay.ex):
                    for ey in range(lay.ey):
                        point = (q1 * 3 + q2) * lay.group + ex * lay.ey + ey
                        for a1 in range(3):
                            for a2 in range(3):
                                p, r = 2 * (ex - 1) + a1, 2 * (ey - 1) + a2
                                factor = tx[q1, a1] * ty[q2, a2]
                                forward[kind, point, lay.row(p, r)] += factor
                                if 0 <= p < lay.nx and 0 <= r < lay.ny:
                                    back[kind, p * lay.ny + r, point] += factor * weights[q1] * weights[q2]
    along_z = np.zeros((2, 2 * lay.nz, lay.lanes))
    z_back = np.zeros((2, lay.lanes, lay.nz))
    inside = [(q3, ez) for q3 in range(3) for ez in range(1, lay.ez - 1)]
    edge = [(q3, ez) for q3 in range(3) for ez in (0, lay.ez - 1)]
    for column, (q3, ez) in enumerate(inside + edge):
        for kind, tz in enumerate((values, slopes)):
            for a3 in range(3):
                z = 2 * (ez - 1) + a3
                if z < 0:
                    k = lay.nz + lay.nz + z
                elif z >= lay.nz:
                    k = lay.nz + z - lay.nz
                else:
                    k = z
                    z_back[kind, column, z] += tz[q3, a3] * weights[q3]
                along_z[kind, k, column] += tz[q3, a3]
    fh, fl = split_np(forward)
    forward = np.concatenate([fh, fh, fl], axis=2)
    bh, bl = split_np(back)
    back = np.concatenate([bh, bl], axis=1)
    first = np.concatenate(along_z[:, : lay.nz, :128], axis=1)
    second = np.concatenate(along_z[:, :, 128:], axis=1)
    first = np.concatenate(split_np(first), axis=0)
    second = np.stack(split_np(second))
    zh, zl = split_np(z_back)
    z_back = np.concatenate([zh, zl], axis=2)
    return forward, back, first, second, z_back


def split(x):
    high = x.astype(bf16)
    return high, (x - high.astype(f32)).astype(bf16)


def dot(a, b):
    return jnp.dot(a, b, preferred_element_type=f32)


def kernel(
    lay, sizes,
    fields, strain_h, material_h, forward_h, back_h, first_h, second_h, z_back_h,
    out, totals_ref,
    ext, extp, strain, material, forward, back, first, second, z_back, grads, flux, middle,
    send_a, recv_a, send_b, recv_b,
    load_sem, const_sem, halo_send, halo_recv, core_send, core_recv,
    a_send, a_recv, b_send, b_recv, far_sem,
):
    n = dict(sizes)
    me = {axis: lax.axis_index(axis) for axis in ("gx", "gy", "gz")}
    nx, ny, nz = lay.nx, lay.ny, lay.nz
    own, rows = lay.own, lay.rows

    def device(**shifts):
        return {
            axis: lax.rem(me[axis] + (shift % n[axis]), n[axis]) for axis, shift in shifts.items()
        }

    load = pltpu.make_async_copy(fields, ext.at[:, 0:own, :], load_sem)
    load.start()

    barrier = pltpu.get_barrier_semaphore()
    near = [device(gx=1), device(gx=-1), device(gy=1), device(gy=-1)]
    near += [device(gx=i, gy=j) for i in (1, -1) for j in (1, -1)] + [device(gz=1)]
    for where in near:
        pl.semaphore_signal(barrier, inc=1, device_id=where, device_id_type=MESH)

    constants = [
        pltpu.make_async_copy(source, target, const_sem.at[i])
        for i, (source, target) in enumerate(
            (
                (first_h, first), (forward_h, forward), (second_h, second), (back_h, back),
                (z_back_h, z_back), (strain_h, strain), (material_h, material),
            )
        )
    ]
    for copy in constants:
        copy.start()
    if rows > lay.used:
        ext[:, lay.used :, :] = jnp.zeros((6, rows - lay.used, nz), f32)

    count = [0]
    sends = []

    def send(source, target, where):
        i = count[0]
        count[0] += 1
        copy = pltpu.make_async_remote_copy(
            src_ref=ext.at[:, source[0] : source[0] + source[1], :],
            dst_ref=ext.at[:, target : target + source[1], :],
            send_sem=halo_send.at[i],
            recv_sem=halo_recv.at[i],
            device_id=where,
            device_id_type=MESH,
        )
        copy.start()
        sends.append(copy)

    load.wait()
    pl.semaphore_wait(barrier, len(near))
    send(((nx - 2) * ny, 2 * ny), lay.xm, device(gx=1))
    send((0, ny), lay.xp, device(gx=-1))
    for p in range(2):
        send(((nx - 2 + p) * ny + ny - 2, 2), lay.ym_xm + 2 * p, device(gx=1, gy=1))
        send(((nx - 2 + p) * ny, 1), lay.yp_xm + p, device(gx=1, gy=-1))
    send((ny - 2, 2), lay.ym_xp, device(gx=-1, gy=1))
    send((0, 1), lay.yp_xp, device(gx=-1, gy=-1))
    for p in range(nx):
        send((p * ny + ny - 2, 2), lay.ym_own + 2 * p, device(gy=1))
        send((p * ny, 1), lay.yp_own + p, device(gy=-1))

    def to_core(i, start, stop):
        return pltpu.make_async_remote_copy(
            src_ref=ext.at[:, start:stop, :],
            dst_ref=extp.at[:, start:stop, :],
            send_sem=core_send.at[i],
            recv_sem=core_recv.at[i],
            device_id=device(gz=1),
            device_id_type=MESH,
        )

    core_own = to_core(0, 0, own)
    core_own.start()

    def greet(step):
        d = 2**step
        for where in (device(gx=d), device(gx=-d), device(gy=d), device(gy=-d)):
            pl.semaphore_signal(far_sem.at[step], inc=1, device_id=where, device_id_type=MESH)

    far = 1
    while 2**far < n["gx"] // 2 or 2**far <= n["gy"] // 2:
        far += 1
    for step in range(far):
        greet(step)
        if step < far - 1:
            pl.semaphore_wait(far_sem.at[step], 4)

    for copy in sends:
        copy.wait()
    core_halo = to_core(1, own, rows)
    core_halo.start()
    for copy in constants:
        copy.wait()

    def to_points(tile, z):
        high, low = split(z)
        for pair in range(3):
            parts = []
            for kind in range(2):
                sides = []
                for c in (2 * pair, 2 * pair + 1):
                    at = (slice(c * rows, c * rows + rows), slice(kind * 128, kind * 128 + 128))
                    sides.append(jnp.concatenate([high[at], low[at], high[at]], axis=0))
                parts.append(jnp.concatenate(sides, axis=1))
            grads[tile, pair, 0] = dot(forward[0], parts[0])
            grads[tile, pair, 1] = dot(forward[1], parts[0])
            grads[tile, pair, 2] = dot(forward[2], parts[1])

    shear, lame = material[0], material[1]
    ratio = lame / shear
    shift = [
        [strain[i, j] + (1.0 if i == j else 0.0) for j in range(3)] for i in range(3)
    ]

    def stresses(tile):
        def points(i, carry):
            for half in range(2):
                block = pl.ds(pl.multiple_of(i * 16 + half * 8, 8), 8)

                def gradient(c, along):
                    return grads[tile, c // 2, along, block, (c % 2) * 128 : (c % 2) * 128 + 128]

                lanes = slice(tile * 128, tile * 128 + 128)
                f = [[gradient(r, c) + shift[r][c] for c in range(3)] for r in range(3)]
                dv = [[gradient(3 + r, c) for c in range(3)] for r in range(3)]
                cof = [
                    [
                        f[(r + 1) % 3][(c + 1) % 3] * f[(r + 2) % 3][(c + 2) % 3]
                        - f[(r + 1) % 3][(c + 2) % 3] * f[(r + 2) % 3][(c + 1) % 3]
                        for c in range(3)
                    ]
                    for r in range(3)
                ]
                det = f[0][0] * cof[0][0] + f[0][1] * cof[0][1] + f[0][2] * cof[0][2]
                inverse = 1.0 / det
                g = [[cof[r][c] * inverse for c in range(3)] for r in range(3)]
                pressure = ratio * jnp.log(det) - 1.0
                for r in range(3):
                    for c in range(3):
                        flux[r, c, block, lanes] = f[r][c] + pressure * g[r][c]
                m = [
                    [
                        g[r][0] * dv[c][0] + g[r][1] * dv[c][1] + g[r][2] * dv[c][2]
                        for c in range(3)
                    ]
                    for r in range(3)
                ]
                trace = ratio * (m[0][0] + m[1][1] + m[2][2])
                w = [
                    [
                        trace - pressure * m[r][c] if r == c else -(pressure * m[r][c])
                        for c in range(3)
                    ]
                    for r in range(3)
                ]
                for r in range(3):
                    for c in range(3):
                        flux[3 + r, c, block, lanes] = dv[r][c] + (
                            w[r][0] * g[0][c] + w[r][1] * g[1][c] + w[r][2] * g[2][c]
                        )
            return carry

        lax.fori_loop(0, lay.points // 16, points, 0)

    nodes = ext[...].reshape(6 * rows, nz)
    high, low = split(nodes)
    weights = first[0:nz]
    z = dot(
        jnp.concatenate([high, low], axis=1), jnp.concatenate([weights, weights], axis=0)
    ) + dot(high, first[nz:])
    to_points(0, z)
    stresses(0)

    core_own.wait()
    core_halo.wait()
    nodes = jnp.concatenate([nodes, extp[...].reshape(6 * rows, nz)], axis=1)
    high, low = split(nodes)
    z = dot(high, second[0]) + dot(low, second[0]) + dot(high, second[1])
    to_points(1, z)
    stresses(1)

    for c in range(6):
        def plane(kind, along):
            high, low = split(flux[c, along])
            both = dot(back[kind], high)
            return both[:own] + both[own:] + dot(back[kind, :own], low)

        at = slice(c * own, c * own + own)
        for kind, part in enumerate((plane(0, 0) + plane(1, 1), plane(2, 2))):
            high, low = split(part)
            middle[kind, 0, at] = high
            middle[kind, 1, at] = low
    result = dot(middle[0, 1], z_back[0, :, :nz]) + dot(middle[1, 1], z_back[1, :, :nz])
    both = dot(middle[0, 0], z_back[0]) + dot(middle[1, 0], z_back[1])
    result = (result + both[:, :nz] + both[:, nz:]) * shear
    out[...] = result
    sums = []
    for c0 in (0, 3):
        total = jnp.zeros((8, nz), f32)
        for c in range(c0, c0 + 3):
            part = result[c * own : c * own + own]
            product = part * (part if c < 3 else ext[c, :own])
            for k in range(own // 8):
                total = total + product[8 * k : 8 * k + 8]
        sums.append(jnp.sum(total, axis=0, keepdims=True))
    totals = jnp.concatenate(sums, axis=0)

    pl.semaphore_wait(far_sem.at[far - 1], 4)

    def exchange(totals, partners, sending, receiving, send_sems, recv_sems):
        sending[...] = totals
        copies = []
        for slot, where in enumerate(partners):
            copy = pltpu.make_async_remote_copy(
                src_ref=sending,
                dst_ref=receiving.at[slot],
                send_sem=send_sems.at[slot],
                recv_sem=recv_sems.at[slot],
                device_id=where,
                device_id_type=MESH,
            )
            copy.start()
            copies.append(copy)
        for copy in copies:
            copy.wait_recv()
        return totals + jnp.sum(receiving[...], axis=0), copies

    half = n["gx"] // 2
    order = [k for d in range(1, half + 1) for k in sorted({d, n["gx"] - d})]
    totals, copies_a = exchange(
        totals, [device(gx=k) for k in order], send_a, recv_a, a_send, a_recv
    )
    half = n["gy"] // 2
    order = [k for d in range(half, 0, -1) for k in sorted({d, n["gy"] - d})] + [0]
    partners = []
    for k in order:
        partners.append(device(gy=k, gz=1))
        if k:
            partners.append(device(gy=k))
    totals, copies_b = exchange(totals, partners, send_b, recv_b, b_send, b_recv)
    totals_ref[...] = totals
    for copy in copies_a + copies_b:
        copy.wait_send()


def finish(entries, out, totals, residual, tangent, stats, held, sems):
    half = out.shape[0] // 2
    copies = [
        pltpu.make_async_copy(out.at[0:half], residual, sems.at[0]),
        pltpu.make_async_copy(out.at[half:], tangent, sems.at[1]),
    ]
    for copy in copies:
        copy.start()
    means = jnp.sum(totals[...], axis=1, keepdims=True) / entries
    root = jnp.sqrt(means + root_eps)
    held[0] = root[0, 0]
    held[1] = means[1, 0]
    copies.append(pltpu.make_async_copy(held, stats, sems.at[2]))
    copies[-1].start()
    for copy in copies:
        copy.wait()


def solution(mesh):
    sizes = tuple((axis, mesh.shape[axis]) for axis in ("gx", "gy", "gz"))
    n = dict(sizes)

    def local(fields, macro_strain, material):
        nx, ny, nz = fields.shape[2:]
        lay = Layout(nx, ny, nz)
        consts = [jnp.asarray(m) for m in matrices(lay)]
        hbm = pl.BlockSpec(memory_space=pltpu.HBM)
        vmem = pl.BlockSpec(memory_space=pltpu.VMEM)
        halos = 2 + 2 * nx + 6
        own = lay.own
        n_a, n_b = n["gx"] - 1, n["gy"] * n["gz"] - 1
        dma = pltpu.SemaphoreType.DMA
        out, totals = pl.pallas_call(
            functools.partial(kernel, lay, sizes),
            out_shape=(
                pltpu.VMEM((6 * own, nz), f32),
                pltpu.VMEM((2, nz), f32),
            ),
            in_specs=[hbm] * 8,
            out_specs=(vmem, vmem),
            scratch_shapes=[
                pltpu.VMEM((6, lay.rows, nz), f32),
                pltpu.VMEM((6, lay.rows, nz), f32),
                pltpu.SMEM(macro_strain.shape, f32),
                pltpu.SMEM(material.shape, f32),
                *[pltpu.VMEM(m.shape, bf16) for m in consts],
                pltpu.VMEM((2, 3, 3, lay.points, 256), f32),
                pltpu.VMEM((6, 3, lay.points, lay.lanes), f32),
                pltpu.VMEM((2, 2, 6 * own, lay.lanes), bf16),
                pltpu.VMEM((2, nz), f32),
                pltpu.VMEM((n_a, 2, nz), f32),
                pltpu.VMEM((2, nz), f32),
                pltpu.VMEM((n_b, 2, nz), f32),
                dma,
                dma((7,)),
                dma((halos,)),
                dma((halos,)),
                dma((2,)),
                dma((2,)),
                dma((n_a,)),
                dma((n_a,)),
                dma((n_b,)),
                dma((n_b,)),
                pltpu.SemaphoreType.REGULAR((8,)),
            ],
            compiler_params=pltpu.CompilerParams(
                collective_id=0, has_side_effects=True
            ),
            name="cell",
        )(fields.reshape(6, nx * ny, nz), macro_strain, material, *consts)
        entries = 3.0 * nx * ny * nz * n["gx"] * n["gy"] * n["gz"]
        block = jax.ShapeDtypeStruct((3 * own, nz), f32)
        residual, tangent, stats = pl.pallas_call(
            functools.partial(finish, entries),
            out_shape=(block, block, jax.ShapeDtypeStruct((2,), f32)),
            in_specs=[vmem, vmem],
            out_specs=(hbm, hbm, hbm),
            scratch_shapes=[pltpu.SMEM((2,), f32), dma((3,))],
            compiler_params=pltpu.CompilerParams(vmem_limit_bytes=24 * 2**20),
            name="finish",
        )(out, totals)
        shape = (3, nx, ny, nz)
        return residual.reshape(shape), tangent.reshape(shape), stats

    in_specs = (P("body", None, "gx", "gy", "gz"), P("body", None), P("body"))
    out_specs = (P("body", "gx", "gy", "gz"), P("body", "gx", "gy", "gz"), P("body"))
    return jax.shard_map(local, mesh=mesh, in_specs=in_specs, out_specs=out_specs, check_vma=False)
```

```python
import functools
import math

import jax
import jax.numpy as jnp
import numpy as np
from jax import lax
from jax.experimental import pallas as pl
from jax.experimental.pallas import tpu as pltpu
from jax.sharding import PartitionSpec as P

MESH = pl.DeviceIdType.MESH
spacing = 4.0
root_eps = 1e-06
f32 = jnp.float32
bf16 = jnp.bfloat16


def tables():
    root = math.sqrt(0.6)
    points = np.array([-root, 0.0, root])
    values = np.stack(
        [points * (points - 1.0) / 2.0, 1.0 - points * points, points * (points + 1.0) / 2.0], axis=1
    )
    slopes = np.stack([points - 0.5, -2.0 * points, points + 0.5], axis=1) * (2.0 / spacing)
    weights = np.array([5.0 / 9.0, 8.0 / 9.0, 5.0 / 9.0]) * (spacing / 2.0)
    return values, slopes, weights


def ceil_to(n, m):
    return -(-n // m) * m


class Layout:
    def __init__(self, nx, ny, nz):
        self.nx, self.ny, self.nz = nx, ny, nz
        self.own = nx * ny
        self.xm = self.own
        self.xp = self.xm + 2 * ny
        self.ym_own = self.xp + ny
        self.ym_xm = self.ym_own + 2 * nx
        self.ym_xp = self.ym_xm + 4
        self.yp_own = self.ym_xp + 2
        self.yp_xm = self.yp_own + nx
        self.yp_xp = self.yp_xm + 2
        self.used = self.yp_xp + 1
        self.rows = ceil_to(self.used, 16)
        self.ex, self.ey, self.ez = nx // 2 + 1, ny // 2 + 1, nz // 2 + 1
        self.group = ceil_to(self.ex * self.ey, 16)
        self.points = 9 * self.group
        self.lanes = ceil_to(3 * self.ez, 128)

    def row(self, p, r):
        if 0 <= r < self.ny:
            if 0 <= p < self.nx:
                return p * self.ny + r
            if p < 0:
                return self.xm + (p + 2) * self.ny + r
            return self.xp + r
        if r < 0:
            if 0 <= p < self.nx:
                return self.ym_own + 2 * p + r + 2
            if p < 0:
                return self.ym_xm + 2 * (p + 2) + r + 2
            return self.ym_xp + r + 2
        if 0 <= p < self.nx:
            return self.yp_own + p
        if p < 0:
            return self.yp_xm + p + 2
        return self.yp_xp


def split_np(a):
    a = a.astype(np.float32)
    high = np.asarray(a, dtype=jnp.bfloat16)
    low = np.asarray(a - high.astype(np.float32), dtype=jnp.bfloat16)
    return high, low


def matrices(lay):
    values, slopes, weights = tables()
    forward = np.zeros((3, lay.points, lay.rows))
    back = np.zeros((3, lay.own, lay.points))
    pairs = ((slopes, values), (values, slopes), (values, values))
    for kind, (tx, ty) in enumerate(pairs):
        for q1 in range(3):
            for q2 in range(3):
                for ex in range(lay.ex):
                    for ey in range(lay.ey):
                        point = (q1 * 3 + q2) * lay.group + ex * lay.ey + ey
                        for a1 in range(3):
                            for a2 in range(3):
                                p, r = 2 * (ex - 1) + a1, 2 * (ey - 1) + a2
                                factor = tx[q1, a1] * ty[q2, a2]
                                forward[kind, point, lay.row(p, r)] += factor
                                if 0 <= p < lay.nx and 0 <= r < lay.ny:
                                    back[kind, p * lay.ny + r, point] += factor * weights[q1] * weights[q2]
    along_z = np.zeros((2, 2 * lay.nz, lay.lanes))
    z_back = np.zeros((2, lay.lanes, lay.nz))
    inside = [(q3, ez) for q3 in range(3) for ez in range(1, lay.ez - 1)]
    edge = [(q3, ez) for q3 in range(3) for ez in (0, lay.ez - 1)]
    for column, (q3, ez) in enumerate(inside + edge):
        for kind, tz in enumerate((values, slopes)):
            for a3 in range(3):
                z = 2 * (ez - 1) + a3
                if z < 0:
                    k = lay.nz + lay.nz + z
                elif z >= lay.nz:
                    k = lay.nz + z - lay.nz
                else:
                    k = z
                    z_back[kind, column, z] += tz[q3, a3] * weights[q3]
                along_z[kind, k, column] += tz[q3, a3]
    fh, fl = split_np(forward)
    forward = np.concatenate([fh, fh, fl], axis=2)
    bh, bl = split_np(back)
    back = np.concatenate([bh, bl], axis=1)
    first = np.concatenate(along_z[:, : lay.nz, :128], axis=1)
    second = np.concatenate(along_z[:, :, 128:], axis=1)
    first = np.concatenate(split_np(first), axis=0)
    second = np.stack(split_np(second))
    zh, zl = split_np(z_back)
    z_back = np.concatenate([zh, zl], axis=2)
    return forward, back, first, second, z_back


def split(x):
    high = x.astype(bf16)
    return high, (x - high.astype(f32)).astype(bf16)


def dot(a, b):
    return jnp.dot(a, b, preferred_element_type=f32)


def kernel(
    lay, sizes,
    fields, strain_h, material_h, forward_h, back_h, first_h, second_h, z_back_h,
    out, totals_ref,
    ext, extp, strain, material, forward, back, first, second, z_back, grads, flux, middle,
    own_row, plane_row, plane_rows, near_rows, far_rows,
    load_sem, const_sem, halo_send, halo_recv, core_send, core_recv,
    plane_send, plane_recv, near_send, near_recv, far_send, far_recv, known_sem,
):
    n = dict(sizes)
    me = {axis: lax.axis_index(axis) for axis in ("gx", "gy", "gz")}
    nx, ny, nz = lay.nx, lay.ny, lay.nz
    own, rows = lay.own, lay.rows

    def device(**shifts):
        return {
            axis: lax.rem(me[axis] + (shift % n[axis]), n[axis]) for axis, shift in shifts.items()
        }

    load = pltpu.make_async_copy(fields, ext.at[:, 0:own, :], load_sem)
    load.start()

    barrier = pltpu.get_barrier_semaphore()
    around = [(1, 1), (1, -1), (-1, 1), (-1, -1), (1, 0), (-1, 0), (0, 1), (0, -1)]
    near = [device(gx=i, gy=j) for i, j in around] + [device(gz=1)]
    near += [device(gx=i, gy=j, gz=1) for i, j in around]
    for where in near:
        pl.semaphore_signal(barrier, inc=1, device_id=where, device_id_type=MESH)

    constants = [
        pltpu.make_async_copy(source, target, const_sem.at[i])
        for i, (source, target) in enumerate(
            (
                (first_h, first), (forward_h, forward), (second_h, second), (back_h, back),
                (z_back_h, z_back), (strain_h, strain), (material_h, material),
            )
        )
    ]
    for copy in constants:
        copy.start()
    if rows > lay.used:
        ext[:, lay.used :, :] = jnp.zeros((6, rows - lay.used, nz), f32)

    count = [0]
    sends = []

    def send(source, target, where):
        i = count[0]
        count[0] += 1
        copy = pltpu.make_async_remote_copy(
            src_ref=ext.at[:, source[0] : source[0] + source[1], :],
            dst_ref=ext.at[:, target : target + source[1], :],
            send_sem=halo_send.at[i],
            recv_sem=halo_recv.at[i],
            device_id=where,
            device_id_type=MESH,
        )
        copy.start()
        sends.append(copy)

    load.wait()
    pl.semaphore_wait(barrier, len(near))
    for p in range(2):
        send(((nx - 2 + p) * ny + ny - 2, 2), lay.ym_xm + 2 * p, device(gx=1, gy=1))
        send(((nx - 2 + p) * ny, 1), lay.yp_xm + p, device(gx=1, gy=-1))
    send((ny - 2, 2), lay.ym_xp, device(gx=-1, gy=1))
    send((0, 1), lay.yp_xp, device(gx=-1, gy=-1))
    send(((nx - 2) * ny, 2 * ny), lay.xm, device(gx=1))
    send((0, ny), lay.xp, device(gx=-1))
    for p in range(nx):
        send((p * ny + ny - 2, 2), lay.ym_own + 2 * p, device(gy=1))
        send((p * ny, 1), lay.yp_own + p, device(gy=-1))

    def to_core(i, start, stop):
        return pltpu.make_async_remote_copy(
            src_ref=ext.at[:, start:stop, :],
            dst_ref=extp.at[:, start:stop, :],
            send_sem=core_send.at[i],
            recv_sem=core_recv.at[i],
            device_id=device(gz=1),
            device_id_type=MESH,
        )

    core_own = to_core(0, 0, own)
    core_own.start()

    rounds = {
        "gx": max(1, math.ceil(math.log2(n["gx"] / 2))), "gy": max(1, math.ceil(math.log2(n["gy"] / 2)))
    }
    last = max(rounds.values())

    def greeted(step):
        return [axis for axis in ("gx", "gy") if step < rounds[axis]]

    for step in range(last):
        for axis in greeted(step):
            for d in (2**step, -(2**step)):
                pl.semaphore_signal(
                    known_sem.at[step], inc=1, device_id=device(**{axis: d}), device_id_type=MESH
                )
        if step < last - 1:
            pl.semaphore_wait(known_sem.at[step], 2 * len(greeted(step)))

    for copy in sends:
        copy.wait()
    core_halo = to_core(1, own, rows)
    core_halo.start()
    for copy in constants:
        copy.wait()

    def to_points(tile, z):
        high, low = split(z)
        for pair in range(3):
            parts = []
            for kind in range(2):
                sides = []
                for c in (2 * pair, 2 * pair + 1):
                    at = (slice(c * rows, c * rows + rows), slice(kind * 128, kind * 128 + 128))
                    sides.append(jnp.concatenate([high[at], low[at], high[at]], axis=0))
                parts.append(jnp.concatenate(sides, axis=1))
            grads[tile, pair, 0] = dot(forward[0], parts[0])
            grads[tile, pair, 1] = dot(forward[1], parts[0])
            grads[tile, pair, 2] = dot(forward[2], parts[1])

    shear, lame = material[0], material[1]
    ratio = lame / shear
    shift = [
        [strain[i, j] + (1.0 if i == j else 0.0) for j in range(3)] for i in range(3)
    ]

    def stresses(tile):
        def points(i, carry):
            for half in range(2):
                block = pl.ds(pl.multiple_of(i * 16 + half * 8, 8), 8)

                def gradient(c, along):
                    return grads[tile, c // 2, along, block, (c % 2) * 128 : (c % 2) * 128 + 128]

                lanes = slice(tile * 128, tile * 128 + 128)
                f = [[gradient(r, c) + shift[r][c] for c in range(3)] for r in range(3)]
                dv = [[gradient(3 + r, c) for c in range(3)] for r in range(3)]
                cof = [
                    [
                        f[(r + 1) % 3][(c + 1) % 3] * f[(r + 2) % 3][(c + 2) % 3]
                        - f[(r + 1) % 3][(c + 2) % 3] * f[(r + 2) % 3][(c + 1) % 3]
                        for c in range(3)
                    ]
                    for r in range(3)
                ]
                det = f[0][0] * cof[0][0] + f[0][1] * cof[0][1] + f[0][2] * cof[0][2]
                inverse = 1.0 / det
                g = [[cof[r][c] * inverse for c in range(3)] for r in range(3)]
                pressure = ratio * jnp.log(det) - 1.0
                for r in range(3):
                    for c in range(3):
                        flux[r, c, block, lanes] = f[r][c] + pressure * g[r][c]
                m = [
                    [
                        g[r][0] * dv[c][0] + g[r][1] * dv[c][1] + g[r][2] * dv[c][2]
                        for c in range(3)
                    ]
                    for r in range(3)
                ]
                trace = ratio * (m[0][0] + m[1][1] + m[2][2])
                w = [
                    [
                        trace - pressure * m[r][c] if r == c else -(pressure * m[r][c])
                        for c in range(3)
                    ]
                    for r in range(3)
                ]
                for r in range(3):
                    for c in range(3):
                        flux[3 + r, c, block, lanes] = dv[r][c] + (
                            w[r][0] * g[0][c] + w[r][1] * g[1][c] + w[r][2] * g[2][c]
                        )
            return carry

        lax.fori_loop(0, lay.points // 16, points, 0)

    nodes = ext[...].reshape(6 * rows, nz)
    high, low = split(nodes)
    weights = first[0:nz]
    z = dot(
        jnp.concatenate([high, low], axis=1), jnp.concatenate([weights, weights], axis=0)
    ) + dot(high, first[nz:])
    to_points(0, z)
    stresses(0)

    core_own.wait()
    core_halo.wait()
    nodes = jnp.concatenate([nodes, extp[...].reshape(6 * rows, nz)], axis=1)
    high, low = split(nodes)
    z = dot(high, second[0]) + dot(low, second[0]) + dot(high, second[1])
    to_points(1, z)
    stresses(1)

    for c in range(6):
        def plane(kind, along):
            high, low = split(flux[c, along])
            both = dot(back[kind], high)
            return both[:own] + both[own:] + dot(back[kind, :own], low)

        at = slice(c * own, c * own + own)
        for kind, part in enumerate((plane(0, 0) + plane(1, 1), plane(2, 2))):
            high, low = split(part)
            middle[kind, 0, at] = high
            middle[kind, 1, at] = low
    result = dot(middle[0, 1], z_back[0, :, :nz]) + dot(middle[1, 1], z_back[1, :, :nz])
    both = dot(middle[0, 0], z_back[0]) + dot(middle[1, 0], z_back[1])
    result = (result + both[:, :nz] + both[:, nz:]) * shear
    out[...] = result
    sums = []
    for c0 in (0, 3):
        total = jnp.zeros((8, nz), f32)
        for c in range(c0, c0 + 3):
            part = result[c * own : c * own + own]
            product = part * (part if c < 3 else ext[c, :own])
            for k in range(own // 8):
                total = total + product[8 * k : 8 * k + 8]
        sums.append(total + pltpu.roll(total, nz // 2, 1))
    lane = lax.broadcasted_iota(jnp.int32, (8, nz), 1)
    folded = jnp.sum(jnp.where(lane < nz // 2, sums[0], sums[1]), axis=0, keepdims=True)
    own_row[...] = folded

    def row_to(source, target, slot, send_sems, recv_sems, where):
        copy = pltpu.make_async_remote_copy(
            src_ref=source,
            dst_ref=target.at[slot : slot + 1],
            send_sem=send_sems.at[slot],
            recv_sem=recv_sems.at[slot],
            device_id=where,
            device_id_type=MESH,
        )
        copy.start()
        return copy

    half = n["gy"] // 2
    if rounds["gy"] >= last:
        pl.semaphore_wait(known_sem.at[last - 1], 2 * len(greeted(last - 1)))
    in_plane, in_near = [], []
    for k in [k for d in range(half, 0, -1) for k in sorted({d, n["gy"] - d})] + [0]:
        for i in beside(n["gx"]):
            for core in (1, 0):
                where = device(gx=i, gy=k, gz=core)
                in_near.append(
                    row_to(own_row, near_rows, len(in_near), near_send, near_recv, where)
                )
        for core in (1, 0):
            if k or core:
                where = device(gy=k, gz=core)
                in_plane.append(
                    row_to(own_row, plane_rows, len(in_plane), plane_send, plane_recv, where)
                )
    for copy in in_plane:
        copy.wait_recv()
    plane_total = folded + jnp.sum(plane_rows[...], axis=0, keepdims=True)
    plane_row[...] = plane_total
    if rounds["gy"] < last:
        pl.semaphore_wait(known_sem.at[last - 1], 2 * len(greeted(last - 1)))
    in_far = [
        row_to(plane_row, far_rows, slot, far_send, far_recv, device(gx=k))
        for slot, k in enumerate(beyond(n["gx"]))
    ]
    for copy in in_near + in_far:
        copy.wait_recv()
    total = plane_total + jnp.sum(near_rows[...], axis=0, keepdims=True)
    if in_far:
        total = total + jnp.sum(far_rows[...], axis=0, keepdims=True)
    totals_ref[...] = total
    for copy in in_plane + in_near + in_far:
        copy.wait_send()


def beside(size):
    return sorted({1, size - 1})


def beyond(size):
    return [k for k in range(1, size) if k not in beside(size)]


def finish(entries, out, totals, residual, tangent, stats, held, sems):
    half = out.shape[0] // 2
    copies = [
        pltpu.make_async_copy(out.at[0:half], residual, sems.at[0]),
        pltpu.make_async_copy(out.at[half:], tangent, sems.at[1]),
    ]
    for copy in copies:
        copy.start()
    row = totals[...]
    first = lax.broadcasted_iota(jnp.int32, row.shape, 1) < row.shape[1] // 2
    squares = jnp.sum(jnp.where(first, row, 0.0), axis=1, keepdims=True) / entries
    curvature = jnp.sum(jnp.where(first, 0.0, row), axis=1, keepdims=True) / entries
    held[0] = jnp.sqrt(squares + root_eps)[0, 0]
    held[1] = curvature[0, 0]
    copies.append(pltpu.make_async_copy(held, stats, sems.at[2]))
    copies[-1].start()
    for copy in copies:
        copy.wait()


def solution(mesh):
    sizes = tuple((axis, mesh.shape[axis]) for axis in ("gx", "gy", "gz"))
    n = dict(sizes)

    def local(fields, macro_strain, material):
        nx, ny, nz = fields.shape[2:]
        lay = Layout(nx, ny, nz)
        consts = [jnp.asarray(m) for m in matrices(lay)]
        hbm = pl.BlockSpec(memory_space=pltpu.HBM)
        vmem = pl.BlockSpec(memory_space=pltpu.VMEM)
        halos = 2 + 2 * nx + 6
        own = lay.own
        plane = n["gy"] * n["gz"]
        near, far = plane * len(beside(n["gx"])), len(beyond(n["gx"]))
        dma = pltpu.SemaphoreType.DMA
        out, totals = pl.pallas_call(
            functools.partial(kernel, lay, sizes),
            out_shape=(
                pltpu.VMEM((6 * own, nz), f32),
                pltpu.VMEM((1, nz), f32),
            ),
            in_specs=[hbm] * 8,
            out_specs=(vmem, vmem),
            scratch_shapes=[
                pltpu.VMEM((6, lay.rows, nz), f32),
                pltpu.VMEM((6, lay.rows, nz), f32),
                pltpu.SMEM(macro_strain.shape, f32),
                pltpu.SMEM(material.shape, f32),
                *[pltpu.VMEM(m.shape, bf16) for m in consts],
                pltpu.VMEM((2, 3, 3, lay.points, 256), f32),
                pltpu.VMEM((6, 3, lay.points, lay.lanes), f32),
                pltpu.VMEM((2, 2, 6 * own, lay.lanes), bf16),
                pltpu.VMEM((1, nz), f32),
                pltpu.VMEM((1, nz), f32),
                pltpu.VMEM((plane - 1, nz), f32),
                pltpu.VMEM((near, nz), f32),
                pltpu.VMEM((max(far, 1), nz), f32),
                dma,
                dma((7,)),
                dma((halos,)),
                dma((halos,)),
                dma((2,)),
                dma((2,)),
                dma((plane - 1,)),
                dma((plane - 1,)),
                dma((near,)),
                dma((near,)),
                dma((max(far, 1),)),
                dma((max(far, 1),)),
                pltpu.SemaphoreType.REGULAR((8,)),
            ],
            compiler_params=pltpu.CompilerParams(
                collective_id=0, has_side_effects=True
            ),
            name="cell",
        )(fields.reshape(6, nx * ny, nz), macro_strain, material, *consts)
        entries = 3.0 * nx * ny * nz * n["gx"] * n["gy"] * n["gz"]
        block = jax.ShapeDtypeStruct((3 * own, nz), f32)
        residual, tangent, stats = pl.pallas_call(
            functools.partial(finish, entries),
            out_shape=(block, block, jax.ShapeDtypeStruct((2,), f32)),
            in_specs=[vmem, vmem],
            out_specs=(hbm, hbm, hbm),
            scratch_shapes=[pltpu.SMEM((2,), f32), dma((3,))],
            compiler_params=pltpu.CompilerParams(vmem_limit_bytes=24 * 2**20),
            name="finish",
        )(out, totals)
        shape = (3, nx, ny, nz)
        return residual.reshape(shape), tangent.reshape(shape), stats

    in_specs = (P("body", None, "gx", "gy", "gz"), P("body", None), P("body"))
    out_specs = (P("body", "gx", "gy", "gz"), P("body", "gx", "gy", "gz"), P("body"))
    return jax.shard_map(local, mesh=mesh, in_specs=in_specs, out_specs=out_specs, check_vma=False)
```

```python
import functools
import math

import jax
import jax.numpy as jnp
import numpy as np
from jax import lax
from jax.experimental import pallas as pl
from jax.experimental.pallas import tpu as pltpu
from jax.sharding import PartitionSpec as P

MESH = pl.DeviceIdType.MESH
spacing = 4.0
root_eps = 1e-06
f32 = jnp.float32
bf16 = jnp.bfloat16


def tables():
    root = math.sqrt(0.6)
    points = np.array([-root, 0.0, root])
    values = np.stack(
        [points * (points - 1.0) / 2.0, 1.0 - points * points, points * (points + 1.0) / 2.0], axis=1
    )
    slopes = np.stack([points - 0.5, -2.0 * points, points + 0.5], axis=1) * (2.0 / spacing)
    weights = np.array([5.0 / 9.0, 8.0 / 9.0, 5.0 / 9.0]) * (spacing / 2.0)
    return values, slopes, weights


def ceil_to(n, m):
    return -(-n // m) * m


class Layout:
    def __init__(self, nx, ny, nz):
        self.nx, self.ny, self.nz = nx, ny, nz
        self.own = nx * ny
        self.xm = self.own
        self.xp = self.xm + 2 * ny
        self.ym_own = self.xp + ny
        self.ym_xm = self.ym_own + 2 * nx
        self.ym_xp = self.ym_xm + 4
        self.yp_own = self.ym_xp + 2
        self.yp_xm = self.yp_own + nx
        self.yp_xp = self.yp_xm + 2
        self.used = self.yp_xp + 1
        self.rows = ceil_to(self.used, 16)
        self.ex, self.ey, self.ez = nx // 2 + 1, ny // 2 + 1, nz // 2 + 1
        self.group = ceil_to(self.ex * self.ey, 16)
        self.points = 9 * self.group
        self.lanes = ceil_to(3 * self.ez, 128)

    def row(self, p, r):
        if 0 <= r < self.ny:
            if 0 <= p < self.nx:
                return p * self.ny + r
            if p < 0:
                return self.xm + (p + 2) * self.ny + r
            return self.xp + r
        if r < 0:
            if 0 <= p < self.nx:
                return self.ym_own + 2 * p + r + 2
            if p < 0:
                return self.ym_xm + 2 * (p + 2) + r + 2
            return self.ym_xp + r + 2
        if 0 <= p < self.nx:
            return self.yp_own + p
        if p < 0:
            return self.yp_xm + p + 2
        return self.yp_xp


def split_np(a):
    a = a.astype(np.float32)
    high = np.asarray(a, dtype=jnp.bfloat16)
    low = np.asarray(a - high.astype(np.float32), dtype=jnp.bfloat16)
    return high, low


def matrices(lay):
    values, slopes, weights = tables()
    forward = np.zeros((3, lay.points, lay.rows))
    back = np.zeros((3, lay.own, lay.points))
    pairs = ((slopes, values), (values, slopes), (values, values))
    for kind, (tx, ty) in enumerate(pairs):
        for q1 in range(3):
            for q2 in range(3):
                for ex in range(lay.ex):
                    for ey in range(lay.ey):
                        point = (q1 * 3 + q2) * lay.group + ex * lay.ey + ey
                        for a1 in range(3):
                            for a2 in range(3):
                                p, r = 2 * (ex - 1) + a1, 2 * (ey - 1) + a2
                                factor = tx[q1, a1] * ty[q2, a2]
                                forward[kind, point, lay.row(p, r)] += factor
                                if 0 <= p < lay.nx and 0 <= r < lay.ny:
                                    back[kind, p * lay.ny + r, point] += factor * weights[q1] * weights[q2]
    along_z = np.zeros((2, 2 * lay.nz, lay.lanes))
    z_back = np.zeros((2, lay.lanes, lay.nz))
    inside = [(q3, ez) for q3 in range(3) for ez in range(1, lay.ez - 1)]
    edge = [(q3, ez) for q3 in range(3) for ez in (0, lay.ez - 1)]
    for column, (q3, ez) in enumerate(inside + edge):
        for kind, tz in enumerate((values, slopes)):
            for a3 in range(3):
                z = 2 * (ez - 1) + a3
                if z < 0:
                    k = lay.nz + lay.nz + z
                elif z >= lay.nz:
                    k = lay.nz + z - lay.nz
                else:
                    k = z
                    z_back[kind, column, z] += tz[q3, a3] * weights[q3]
                along_z[kind, k, column] += tz[q3, a3]
    fh, fl = split_np(forward)
    forward = np.concatenate([fh, fh, fl], axis=2)
    bh, bl = split_np(back)
    back = np.concatenate([bh, bl], axis=1)
    first = np.concatenate(along_z[:, : lay.nz, :128], axis=1)
    second = np.concatenate(along_z[:, :, 128:], axis=1)
    first = np.concatenate(split_np(first), axis=0)
    second = np.stack(split_np(second))
    zh, zl = split_np(z_back)
    z_back = np.concatenate([zh, zl], axis=2)
    return forward, back, first, second, z_back


def split(x):
    high = x.astype(bf16)
    return high, (x - high.astype(f32)).astype(bf16)


def dot(a, b):
    return jnp.dot(a, b, preferred_element_type=f32)


def kernel(
    lay, sizes,
    fields, strain_h, material_h, forward_h, back_h, first_h, second_h, z_back_h,
    out, totals_ref,
    ext, extp, strain, material, forward, back, first, second, z_back, grads, flux, middle,
    own_row, plane_row, plane_rows, near_rows, far_rows,
    load_sem, const_sem, halo_send, halo_recv, core_send, core_recv,
    plane_send, plane_recv, near_send, near_recv, far_send, far_recv, known_sem,
):
    n = dict(sizes)
    me = {axis: lax.axis_index(axis) for axis in ("gx", "gy", "gz")}
    nx, ny, nz = lay.nx, lay.ny, lay.nz
    own, rows = lay.own, lay.rows

    def device(**shifts):
        return {
            axis: lax.rem(me[axis] + (shift % n[axis]), n[axis]) for axis, shift in shifts.items()
        }

    load = pltpu.make_async_copy(fields, ext.at[:, 0:own, :], load_sem)
    load.start()

    barrier = pltpu.get_barrier_semaphore()
    around = [(1, 1), (1, -1), (-1, 1), (-1, -1), (1, 0), (-1, 0), (0, 1), (0, -1)]
    near = [device(gx=i, gy=j) for i, j in around] + [device(gz=1)]
    near += [device(gx=i, gy=j, gz=1) for i, j in around]
    for where in near:
        pl.semaphore_signal(barrier, inc=1, device_id=where, device_id_type=MESH)

    constants = [
        pltpu.make_async_copy(source, target, const_sem.at[i])
        for i, (source, target) in enumerate(
            (
                (first_h, first), (forward_h, forward), (second_h, second), (back_h, back),
                (z_back_h, z_back), (strain_h, strain), (material_h, material),
            )
        )
    ]
    for copy in constants:
        copy.start()
    if rows > lay.used:
        ext[:, lay.used :, :] = jnp.zeros((6, rows - lay.used, nz), f32)

    count = [0]
    sends = []

    def send(source, target, where):
        i = count[0]
        count[0] += 1
        copy = pltpu.make_async_remote_copy(
            src_ref=ext.at[:, source[0] : source[0] + source[1], :],
            dst_ref=ext.at[:, target : target + source[1], :],
            send_sem=halo_send.at[i],
            recv_sem=halo_recv.at[i],
            device_id=where,
            device_id_type=MESH,
        )
        copy.start()
        sends.append(copy)

    load.wait()
    pl.semaphore_wait(barrier, len(near))
    for p in range(2):
        send(((nx - 2 + p) * ny + ny - 2, 2), lay.ym_xm + 2 * p, device(gx=1, gy=1))
        send(((nx - 2 + p) * ny, 1), lay.yp_xm + p, device(gx=1, gy=-1))
    send((ny - 2, 2), lay.ym_xp, device(gx=-1, gy=1))
    send((0, 1), lay.yp_xp, device(gx=-1, gy=-1))
    send(((nx - 2) * ny, 2 * ny), lay.xm, device(gx=1))
    send((0, ny), lay.xp, device(gx=-1))
    for p in range(nx):
        send((p * ny + ny - 2, 2), lay.ym_own + 2 * p, device(gy=1))
        send((p * ny, 1), lay.yp_own + p, device(gy=-1))

    def to_core(i, start, stop):
        return pltpu.make_async_remote_copy(
            src_ref=ext.at[:, start:stop, :],
            dst_ref=extp.at[:, start:stop, :],
            send_sem=core_send.at[i],
            recv_sem=core_recv.at[i],
            device_id=device(gz=1),
            device_id_type=MESH,
        )

    core_own = to_core(0, 0, own)
    core_own.start()

    rounds = {
        "gx": max(1, math.ceil(math.log2(n["gx"] / 2))), "gy": max(1, math.ceil(math.log2(n["gy"] / 2)))
    }
    last = max(rounds.values())

    def greeted(step):
        shifts = [(axis, 2**step) for axis in ("gx", "gy") if step < rounds[axis]]
        if step == last - 1 and step:
            shifts.append(("gx", 2 ** (step - 1)))
        return shifts

    for step in range(last):
        for axis, d in greeted(step):
            for shift in (d, -d):
                pl.semaphore_signal(
                    known_sem.at[step], inc=1, device_id=device(**{axis: shift}), device_id_type=MESH
                )
        if step < last - 1:
            pl.semaphore_wait(known_sem.at[step], 2 * len(greeted(step)))

    for copy in sends:
        copy.wait()
    core_halo = to_core(1, own, rows)
    core_halo.start()
    for copy in constants:
        copy.wait()

    def to_points(tile, z):
        high, low = split(z)
        for pair in range(3):
            parts = []
            for kind in range(2):
                sides = []
                for c in (2 * pair, 2 * pair + 1):
                    at = (slice(c * rows, c * rows + rows), slice(kind * 128, kind * 128 + 128))
                    sides.append(jnp.concatenate([high[at], low[at], high[at]], axis=0))
                parts.append(jnp.concatenate(sides, axis=1))
            grads[tile, pair, 0] = dot(forward[0], parts[0])
            grads[tile, pair, 1] = dot(forward[1], parts[0])
            grads[tile, pair, 2] = dot(forward[2], parts[1])

    shear, lame = material[0], material[1]
    ratio = lame / shear
    shift = [
        [strain[i, j] + (1.0 if i == j else 0.0) for j in range(3)] for i in range(3)
    ]

    def stresses(tile):
        def points(i, carry):
            for half in range(2):
                block = pl.ds(pl.multiple_of(i * 16 + half * 8, 8), 8)

                def gradient(c, along):
                    return grads[tile, c // 2, along, block, (c % 2) * 128 : (c % 2) * 128 + 128]

                lanes = slice(tile * 128, tile * 128 + 128)
                f = [[gradient(r, c) + shift[r][c] for c in range(3)] for r in range(3)]
                dv = [[gradient(3 + r, c) for c in range(3)] for r in range(3)]
                cof = [
                    [
                        f[(r + 1) % 3][(c + 1) % 3] * f[(r + 2) % 3][(c + 2) % 3]
                        - f[(r + 1) % 3][(c + 2) % 3] * f[(r + 2) % 3][(c + 1) % 3]
                        for c in range(3)
                    ]
                    for r in range(3)
                ]
                det = f[0][0] * cof[0][0] + f[0][1] * cof[0][1] + f[0][2] * cof[0][2]
                inverse = 1.0 / det
                g = [[cof[r][c] * inverse for c in range(3)] for r in range(3)]
                pressure = ratio * jnp.log(det) - 1.0
                for r in range(3):
                    for c in range(3):
                        flux[r, c, block, lanes] = f[r][c] + pressure * g[r][c]
                m = [
                    [
                        g[r][0] * dv[c][0] + g[r][1] * dv[c][1] + g[r][2] * dv[c][2]
                        for c in range(3)
                    ]
                    for r in range(3)
                ]
                trace = ratio * (m[0][0] + m[1][1] + m[2][2])
                w = [
                    [
                        trace - pressure * m[r][c] if r == c else -(pressure * m[r][c])
                        for c in range(3)
                    ]
                    for r in range(3)
                ]
                for r in range(3):
                    for c in range(3):
                        flux[3 + r, c, block, lanes] = dv[r][c] + (
                            w[r][0] * g[0][c] + w[r][1] * g[1][c] + w[r][2] * g[2][c]
                        )
            return carry

        lax.fori_loop(0, lay.points // 16, points, 0)

    nodes = ext[...].reshape(6 * rows, nz)
    high, low = split(nodes)
    weights = first[0:nz]
    z = dot(
        jnp.concatenate([high, low], axis=1), jnp.concatenate([weights, weights], axis=0)
    ) + dot(high, first[nz:])
    to_points(0, z)
    stresses(0)

    core_own.wait()
    core_halo.wait()
    nodes = jnp.concatenate([nodes, extp[...].reshape(6 * rows, nz)], axis=1)
    high, low = split(nodes)
    z = dot(high, second[0]) + dot(low, second[0]) + dot(high, second[1])
    to_points(1, z)
    stresses(1)

    for c in range(6):
        def plane(kind, along):
            high, low = split(flux[c, along])
            both = dot(back[kind], high)
            return both[:own] + both[own:] + dot(back[kind, :own], low)

        at = slice(c * own, c * own + own)
        for kind, part in enumerate((plane(0, 0) + plane(1, 1), plane(2, 2))):
            high, low = split(part)
            middle[kind, 0, at] = high
            middle[kind, 1, at] = low
    result = dot(middle[0, 1], z_back[0, :, :nz]) + dot(middle[1, 1], z_back[1, :, :nz])
    both = dot(middle[0, 0], z_back[0]) + dot(middle[1, 0], z_back[1])
    result = (result + both[:, :nz] + both[:, nz:]) * shear
    out[...] = result
    sums = []
    for c0 in (0, 3):
        total = jnp.zeros((8, nz), f32)
        for c in range(c0, c0 + 3):
            part = result[c * own : c * own + own]
            product = part * (part if c < 3 else ext[c, :own])
            for k in range(own // 8):
                total = total + product[8 * k : 8 * k + 8]
        sums.append(total + pltpu.roll(total, nz // 2, 1))
    lane = lax.broadcasted_iota(jnp.int32, (8, nz), 1)
    folded = jnp.sum(jnp.where(lane < nz // 2, sums[0], sums[1]), axis=0, keepdims=True)
    own_row[...] = folded

    def row_to(source, target, slot, send_sem, recv_sem, where):
        pltpu.make_async_remote_copy(
            src_ref=source,
            dst_ref=target.at[slot : slot + 1],
            send_sem=send_sem,
            recv_sem=recv_sem,
            device_id=where,
            device_id_type=MESH,
        ).start()

    def wait_rows(rows, sem):
        pltpu.make_async_copy(rows, rows, sem).wait()

    half = n["gy"] // 2
    order = [k for d in range(half, 0, -1) for k in sorted({d, n["gy"] - d})] + [0]
    slot_near = slot_plane = 0
    for planes in ((1, 0), (2, 3)):
        if planes[0] == 2:
            pl.semaphore_wait(known_sem.at[last - 1], 2 * len(greeted(last - 1)))
        for k in order:
            for i in planes:
                for core in (1, 0):
                    where = device(gx=i, gy=k, gz=core)
                    if i in above(n["gx"]):
                        row_to(own_row, near_rows, slot_near, near_send, near_recv, where)
                        slot_near += 1
                    elif i == 0 and (k or core):
                        row_to(own_row, plane_rows, slot_plane, plane_send, plane_recv, where)
                        slot_plane += 1
    wait_rows(plane_rows, plane_recv)
    plane_total = folded + jnp.sum(plane_rows[...], axis=0, keepdims=True)
    plane_row[...] = plane_total
    far = beyond(n["gx"])
    for slot, k in enumerate(far):
        row_to(plane_row, far_rows, slot, far_send, far_recv, device(gx=k))
    wait_rows(near_rows, near_recv)
    total = plane_total + jnp.sum(near_rows[...], axis=0, keepdims=True)
    if far:
        wait_rows(far_rows, far_recv)
        total = total + jnp.sum(far_rows[...], axis=0, keepdims=True)
    totals_ref[...] = total
    wait_rows(plane_rows, plane_send)
    wait_rows(near_rows, near_send)
    if far:
        wait_rows(far_rows, far_send)


def above(size):
    return range(1, min(size, 4))


def beyond(size):
    return range(4, size)


def finish(entries, out, totals, residual, tangent, stats, held, sems):
    half = out.shape[0] // 2
    copies = [
        pltpu.make_async_copy(out.at[0:half], residual, sems.at[0]),
        pltpu.make_async_copy(out.at[half:], tangent, sems.at[1]),
    ]
    for copy in copies:
        copy.start()
    row = totals[...]
    first = lax.broadcasted_iota(jnp.int32, row.shape, 1) < row.shape[1] // 2
    squares = jnp.sum(jnp.where(first, row, 0.0), axis=1, keepdims=True) / entries
    curvature = jnp.sum(jnp.where(first, 0.0, row), axis=1, keepdims=True) / entries
    held[0] = jnp.sqrt(squares + root_eps)[0, 0]
    held[1] = curvature[0, 0]
    copies.append(pltpu.make_async_copy(held, stats, sems.at[2]))
    copies[-1].start()
    for copy in copies:
        copy.wait()


def solution(mesh):
    sizes = tuple((axis, mesh.shape[axis]) for axis in ("gx", "gy", "gz"))
    n = dict(sizes)

    def local(fields, macro_strain, material):
        nx, ny, nz = fields.shape[2:]
        lay = Layout(nx, ny, nz)
        consts = [jnp.asarray(m) for m in matrices(lay)]
        hbm = pl.BlockSpec(memory_space=pltpu.HBM)
        vmem = pl.BlockSpec(memory_space=pltpu.VMEM)
        halos = 2 + 2 * nx + 6
        own = lay.own
        plane = n["gy"] * n["gz"]
        near, far = plane * len(above(n["gx"])), len(beyond(n["gx"]))
        dma = pltpu.SemaphoreType.DMA
        out, totals = pl.pallas_call(
            functools.partial(kernel, lay, sizes),
            out_shape=(
                pltpu.VMEM((6 * own, nz), f32),
                pltpu.VMEM((1, nz), f32),
            ),
            in_specs=[hbm] * 8,
            out_specs=(vmem, vmem),
            scratch_shapes=[
                pltpu.VMEM((6, lay.rows, nz), f32),
                pltpu.VMEM((6, lay.rows, nz), f32),
                pltpu.SMEM(macro_strain.shape, f32),
                pltpu.SMEM(material.shape, f32),
                *[pltpu.VMEM(m.shape, bf16) for m in consts],
                pltpu.VMEM((2, 3, 3, lay.points, 256), f32),
                pltpu.VMEM((6, 3, lay.points, lay.lanes), f32),
                pltpu.VMEM((2, 2, 6 * own, lay.lanes), bf16),
                pltpu.VMEM((1, nz), f32),
                pltpu.VMEM((1, nz), f32),
                pltpu.VMEM((plane - 1, nz), f32),
                pltpu.VMEM((near, nz), f32),
                pltpu.VMEM((max(far, 1), nz), f32),
                dma,
                dma((7,)),
                dma((halos,)),
                dma((halos,)),
                dma((2,)),
                dma((2,)),
                *[dma] * 6,
                pltpu.SemaphoreType.REGULAR((8,)),
            ],
            compiler_params=pltpu.CompilerParams(
                collective_id=0, has_side_effects=True
            ),
            name="cell",
        )(fields.reshape(6, nx * ny, nz), macro_strain, material, *consts)
        entries = 3.0 * nx * ny * nz * n["gx"] * n["gy"] * n["gz"]
        block = jax.ShapeDtypeStruct((3 * own, nz), f32)
        residual, tangent, stats = pl.pallas_call(
            functools.partial(finish, entries),
            out_shape=(block, block, jax.ShapeDtypeStruct((2,), f32)),
            in_specs=[vmem, vmem],
            out_specs=(hbm, hbm, hbm),
            scratch_shapes=[pltpu.SMEM((2,), f32), dma((3,))],
            compiler_params=pltpu.CompilerParams(vmem_limit_bytes=24 * 2**20),
            name="finish",
        )(out, totals)
        shape = (3, nx, ny, nz)
        return residual.reshape(shape), tangent.reshape(shape), stats

    in_specs = (P("body", None, "gx", "gy", "gz"), P("body", None), P("body"))
    out_specs = (P("body", "gx", "gy", "gz"), P("body", "gx", "gy", "gz"), P("body"))
    return jax.shard_map(local, mesh=mesh, in_specs=in_specs, out_specs=out_specs, check_vma=False)
```

```python
import functools
import math

import jax
import jax.numpy as jnp
import numpy as np
from jax import lax
from jax.experimental import pallas as pl
from jax.experimental.pallas import tpu as pltpu
from jax.sharding import PartitionSpec as P

MESH = pl.DeviceIdType.MESH
spacing = 4.0
root_eps = 1e-06
f32 = jnp.float32
bf16 = jnp.bfloat16


def tables():
    root = math.sqrt(0.6)
    points = np.array([-root, 0.0, root])
    values = np.stack(
        [points * (points - 1.0) / 2.0, 1.0 - points * points, points * (points + 1.0) / 2.0], axis=1
    )
    slopes = np.stack([points - 0.5, -2.0 * points, points + 0.5], axis=1) * (2.0 / spacing)
    weights = np.array([5.0 / 9.0, 8.0 / 9.0, 5.0 / 9.0]) * (spacing / 2.0)
    return values, slopes, weights


def ceil_to(n, m):
    return -(-n // m) * m


class Layout:
    def __init__(self, nx, ny, nz):
        self.nx, self.ny, self.nz = nx, ny, nz
        self.own = nx * ny
        self.xm = self.own
        self.xp = self.xm + 2 * ny
        self.ym_own = self.xp + ny
        self.yp_own = self.ym_own + 2 * nx
        self.corners = self.yp_own + nx
        self.ym_xm = self.corners
        self.ym_xp = self.ym_xm + 4
        self.yp_xm = self.ym_xp + 2
        self.yp_xp = self.yp_xm + 2
        self.used = self.yp_xp + 1
        self.rows = ceil_to(self.used, 16)
        self.ex, self.ey, self.ez = nx // 2 + 1, ny // 2 + 1, nz // 2 + 1
        self.group = ceil_to(self.ex * self.ey, 16)
        self.points = 9 * self.group
        self.lanes = ceil_to(3 * self.ez, 128)

    def row(self, p, r):
        if 0 <= r < self.ny:
            if 0 <= p < self.nx:
                return p * self.ny + r
            if p < 0:
                return self.xm + (p + 2) * self.ny + r
            return self.xp + r
        if r < 0:
            if 0 <= p < self.nx:
                return self.ym_own + 2 * p + r + 2
            if p < 0:
                return self.ym_xm + 2 * (p + 2) + r + 2
            return self.ym_xp + r + 2
        if 0 <= p < self.nx:
            return self.yp_own + p
        if p < 0:
            return self.yp_xm + p + 2
        return self.yp_xp


def split_np(a):
    a = a.astype(np.float32)
    high = np.asarray(a, dtype=jnp.bfloat16)
    low = np.asarray(a - high.astype(np.float32), dtype=jnp.bfloat16)
    return high, low


def matrices(lay):
    values, slopes, weights = tables()
    forward = np.zeros((3, lay.points, lay.rows))
    back = np.zeros((3, lay.own, lay.points))
    pairs = ((slopes, values), (values, slopes), (values, values))
    for kind, (tx, ty) in enumerate(pairs):
        for q1 in range(3):
            for q2 in range(3):
                for ex in range(lay.ex):
                    for ey in range(lay.ey):
                        point = (q1 * 3 + q2) * lay.group + ex * lay.ey + ey
                        for a1 in range(3):
                            for a2 in range(3):
                                p, r = 2 * (ex - 1) + a1, 2 * (ey - 1) + a2
                                factor = tx[q1, a1] * ty[q2, a2]
                                forward[kind, point, lay.row(p, r)] += factor
                                if 0 <= p < lay.nx and 0 <= r < lay.ny:
                                    back[kind, p * lay.ny + r, point] += factor * weights[q1] * weights[q2]
    along_z = np.zeros((2, 2 * lay.nz, lay.lanes))
    z_back = np.zeros((2, lay.lanes, lay.nz))
    inside = [(q3, ez) for q3 in range(3) for ez in range(1, lay.ez - 1)]
    edge = [(q3, ez) for q3 in range(3) for ez in (0, lay.ez - 1)]
    for column, (q3, ez) in enumerate(inside + edge):
        for kind, tz in enumerate((values, slopes)):
            for a3 in range(3):
                z = 2 * (ez - 1) + a3
                if z < 0:
                    k = lay.nz + lay.nz + z
                elif z >= lay.nz:
                    k = lay.nz + z - lay.nz
                else:
                    k = z
                    z_back[kind, column, z] += tz[q3, a3] * weights[q3]
                along_z[kind, k, column] += tz[q3, a3]
    fh, fl = split_np(forward)
    forward = np.concatenate([fh, fh, fl], axis=2).reshape(3 * lay.points, 3 * lay.rows)
    bh, bl = split_np(back)
    back = np.concatenate([bh, bl], axis=1)
    first = np.concatenate(along_z[:, : lay.nz, :128], axis=1)
    second = np.concatenate(along_z[:, :, 128:], axis=1)
    first = np.concatenate(split_np(first), axis=0)
    second = np.stack(split_np(second))
    zh, zl = split_np(z_back)
    z_back = np.concatenate([zh, zl], axis=2)
    return forward, back, first, second, z_back


def split(x):
    high = x.astype(bf16)
    return high, (x - high.astype(f32)).astype(bf16)


def dot(a, b):
    return jnp.dot(a, b, preferred_element_type=f32)


def kernel(
    lay, sizes,
    fields, strain_h, material_h, forward_h, back_h, first_h, second_h, z_back_h,
    out, totals_ref,
    ext, extp, strain, material, forward, back, first, second, z_back, grads, flux, middle,
    own_row, plane_row, plane_rows, near_rows, far_rows,
    load_sem, const_sem, halo_send, halo_recv, core_send, core_recv,
    plane_send, plane_recv, near_send, near_recv, far_send, far_recv, known_sem,
):
    n = dict(sizes)
    me = {axis: lax.axis_index(axis) for axis in ("gx", "gy", "gz")}
    nx, ny, nz = lay.nx, lay.ny, lay.nz
    own, rows = lay.own, lay.rows

    def device(**shifts):
        return {
            axis: lax.rem(me[axis] + (shift % n[axis]), n[axis]) for axis, shift in shifts.items()
        }

    load = pltpu.make_async_copy(fields, ext.at[:, 0:own, :], load_sem)
    load.start()

    barrier = pltpu.get_barrier_semaphore()
    around = [(1, 1), (1, -1), (-1, 1), (-1, -1), (1, 0), (-1, 0), (0, 1), (0, -1)]
    near = [device(gx=i, gy=j) for i, j in around] + [device(gz=1)]
    near += [device(gx=i, gy=j, gz=1) for i, j in around]
    for where in near:
        pl.semaphore_signal(barrier, inc=1, device_id=where, device_id_type=MESH)

    constants = [
        pltpu.make_async_copy(source, target, const_sem.at[i])
        for i, (source, target) in enumerate(
            (
                (first_h, first), (forward_h, forward), (second_h, second), (back_h, back),
                (z_back_h, z_back), (strain_h, strain), (material_h, material),
            )
        )
    ]
    for copy in constants:
        copy.start()
    if rows > lay.used:
        for target in (ext, extp):
            target[:, lay.used :, :] = jnp.zeros((6, rows - lay.used, nz), f32)

    def along_first(nodes):
        high, low = split(nodes)
        weights = first[0:nz]
        return dot(
            jnp.concatenate([high, low], axis=1), jnp.concatenate([weights, weights], axis=0)
        ) + dot(high, first[nz:])

    def along_second(mine, other):
        high, low = split(jnp.concatenate([mine, other], axis=1))
        return dot(high, second[0]) + dot(low, second[0]) + dot(high, second[1])

    count = [0]
    sends = []

    def send(source, target, where, into=ext):
        i = count[0]
        count[0] += 1
        copy = pltpu.make_async_remote_copy(
            src_ref=ext.at[:, source[0] : source[0] + source[1], :],
            dst_ref=into.at[:, target : target + source[1], :],
            send_sem=halo_send.at[i],
            recv_sem=halo_recv.at[i],
            device_id=where,
            device_id_type=MESH,
        )
        copy.start()
        sends.append(copy)

    load.wait()
    pl.semaphore_wait(barrier, len(near))
    for core, into in enumerate((ext, extp)):
        for p in range(2):
            start = (nx - 2 + p) * ny
            send((start + ny - 2, 2), lay.ym_xm + 2 * p, device(gx=1, gy=1, gz=core), into)
            send((start, 1), lay.yp_xm + p, device(gx=1, gy=-1, gz=core), into)
        send((ny - 2, 2), lay.ym_xp, device(gx=-1, gy=1, gz=core), into)
        send((0, 1), lay.yp_xp, device(gx=-1, gy=-1, gz=core), into)
    send(((nx - 2) * ny, 2 * ny), lay.xm, device(gx=1))
    send((0, ny), lay.xp, device(gx=-1))
    for p in range(nx):
        send((p * ny + ny - 2, 2), lay.ym_own + 2 * p, device(gy=1))
        send((p * ny, 1), lay.yp_own + p, device(gy=-1))

    def to_core(i, start, stop):
        return pltpu.make_async_remote_copy(
            src_ref=ext.at[:, start:stop, :],
            dst_ref=extp.at[:, start:stop, :],
            send_sem=core_send.at[i],
            recv_sem=core_recv.at[i],
            device_id=device(gz=1),
            device_id_type=MESH,
        )

    core_own = to_core(0, 0, own)
    core_own.start()

    rounds = {
        "gx": max(1, math.ceil(math.log2(n["gx"] / 2))), "gy": max(1, math.ceil(math.log2(n["gy"] / 2)))
    }
    last = max(rounds.values())

    def greeted(step):
        shifts = [(axis, 2**step) for axis in ("gx", "gy") if step < rounds[axis]]
        if step == last - 1 and step:
            shifts.append(("gx", 2 ** (step - 1)))
        return shifts

    def greet(step):
        for axis, d in greeted(step):
            for shift in (d, -d):
                pl.semaphore_signal(
                    known_sem.at[step], inc=1, device_id=device(**{axis: shift}), device_id_type=MESH
                )

    def next_round(step):
        pl.semaphore_wait(known_sem.at[step], 2 * len(greeted(step)))
        greet(step + 1)

    here, top = me["gx"], n["gx"] - 1
    at_end = (here >= top - 2) | (here <= 1)
    greet(0)
    for step in range(last - 2):
        next_round(step)
    if last > 1:
        @pl.when(at_end)
        def _():
            next_round(last - 2)

    for copy in constants:
        copy.wait()
    own_nodes = ext[:, :own].reshape(6 * own, nz)
    z_own = along_first(own_nodes)
    core_own.wait()
    z_own_second = along_second(own_nodes, extp[:, :own].reshape(6 * own, nz))
    for copy in sends[12:]:
        copy.wait()
    core_halo = to_core(1, own, lay.corners)
    core_halo.start()
    for copy in sends[:12]:
        copy.wait()

    def to_points(tile, z_mine, z_halo):
        mine, halo = split(z_mine), split(z_halo)
        rest = rows - own

        def one(pair):
            parts = []
            for kind in range(2):
                sides = []
                lanes = slice(kind * 128, kind * 128 + 128)
                for c in (2 * pair, 2 * pair + 1):
                    high, low = (
                        jnp.concatenate(
                            [a[c * own : c * own + own, lanes], b[c * rest : c * rest + rest, lanes]],
                            axis=0,
                        )
                        for a, b in zip(mine, halo)
                    )
                    sides.append(jnp.concatenate([high, low, high], axis=0))
                parts.append(jnp.concatenate(sides, axis=1))
            both = dot(forward[: 2 * lay.points], parts[0])
            grads[tile, pair, 0] = both[: lay.points]
            grads[tile, pair, 1] = both[lay.points :]
            grads[tile, pair, 2] = dot(forward[2 * lay.points :], parts[1])

        return one

    shear, lame = material[0], material[1]
    ratio = lame / shear
    shift = [
        [strain[i, j] + (1.0 if i == j else 0.0) for j in range(3)] for i in range(3)
    ]

    def side(c):
        return slice((c % 2) * 128, (c % 2) * 128 + 128)

    def stresses(tile):
        def points(i, carry):
            for half in range(2):
                if isinstance(i, int):
                    block = slice(i * 16 + half * 8, i * 16 + half * 8 + 8)
                else:
                    block = pl.ds(pl.multiple_of(i * 16 + half * 8, 8), 8)

                def gradient(c, along):
                    return grads[tile, c // 2, along, block, side(c)]

                f = [[gradient(r, c) + shift[r][c] for c in range(3)] for r in range(3)]
                dv = [[gradient(3 + r, c) for c in range(3)] for r in range(3)]
                cof = [
                    [
                        f[(r + 1) % 3][(c + 1) % 3] * f[(r + 2) % 3][(c + 2) % 3]
                        - f[(r + 1) % 3][(c + 2) % 3] * f[(r + 2) % 3][(c + 1) % 3]
                        for c in range(3)
                    ]
                    for r in range(3)
                ]
                det = f[0][0] * cof[0][0] + f[0][1] * cof[0][1] + f[0][2] * cof[0][2]
                inverse = 1.0 / det
                g = [[cof[r][c] * inverse for c in range(3)] for r in range(3)]
                pressure = ratio * jnp.log(det) - 1.0
                soft = -pressure
                for r in range(3):
                    for c in range(3):
                        flux[tile, r // 2, c, block, side(r)] = f[r][c] + pressure * g[r][c]
                m = [
                    [
                        g[r][0] * dv[c][0] + g[r][1] * dv[c][1] + g[r][2] * dv[c][2]
                        for c in range(3)
                    ]
                    for r in range(3)
                ]
                trace = ratio * (m[0][0] + m[1][1] + m[2][2])
                w = [
                    [trace + soft * m[r][c] if r == c else soft * m[r][c] for c in range(3)]
                    for r in range(3)
                ]
                for r in range(3):
                    for c in range(3):
                        flux[tile, (3 + r) // 2, c, block, side(3 + r)] = dv[r][c] + (
                            w[r][0] * g[0][c] + w[r][1] * g[1][c] + w[r][2] * g[2][c]
                        )
            return carry

        return points

    rest = 6 * (rows - own)
    halo_nodes = ext[:, own:].reshape(rest, nz)
    def back_pair(tile, pair):
        def plane(kind, along):
            high, low = split(flux[tile, pair, along])
            both = dot(back[kind], high)
            return both[:own] + both[own:] + dot(back[kind, :own], low)

        for kind, part in enumerate((plane(0, 0) + plane(1, 1), plane(2, 2))):
            for hl, piece in enumerate(split(part)):
                for c in (2 * pair, 2 * pair + 1):
                    at = slice(c * own, c * own + own)
                    middle[kind, hl, at, tile * 128 : tile * 128 + 128] = piece[:, side(c)]

    points_of = to_points(0, z_own, along_first(halo_nodes))
    for pair in range(3):
        points_of(pair)
    core_halo.wait()
    points_of = to_points(1, z_own_second, along_second(halo_nodes, extp[:, own:].reshape(rest, nz)))
    blocks = lay.points // 16
    for tile in range(2):
        stress = stresses(tile)
        for i in range(blocks):
            if i % (blocks // 3) == 0:
                pair = i // (blocks // 3)
                if tile == 0:
                    points_of(pair)
                else:
                    back_pair(0, pair)
            stress(i, 0)
    for pair in range(3):
        back_pair(1, pair)
    result = dot(middle[0, 1], z_back[0, :, :nz]) + dot(middle[1, 1], z_back[1, :, :nz])
    both = dot(middle[0, 0], z_back[0]) + dot(middle[1, 0], z_back[1])
    result = (result + both[:, :nz] + both[:, nz:]) * shear
    out[...] = result
    sums = []
    for c0 in (0, 3):
        total = jnp.zeros((8, nz), f32)
        for c in range(c0, c0 + 3):
            part = result[c * own : c * own + own]
            product = part * (part if c < 3 else ext[c, :own])
            for k in range(own // 8):
                total = total + product[8 * k : 8 * k + 8]
        sums.append(total + pltpu.roll(total, nz // 2, 1))
    lane = lax.broadcasted_iota(jnp.int32, (8, nz), 1)
    folded = jnp.sum(jnp.where(lane < nz // 2, sums[0], sums[1]), axis=0, keepdims=True)
    own_row[...] = folded

    def row_to(source, target, slot, send_sem, recv_sem, where):
        pltpu.make_async_remote_copy(
            src_ref=source,
            dst_ref=target.at[slot : slot + 1],
            send_sem=send_sem,
            recv_sem=recv_sem,
            device_id=where,
            device_id_type=MESH,
        ).start()

    def wait_rows(rows, sem):
        pltpu.make_async_copy(rows, rows, sem).wait()

    half = n["gy"] // 2
    order = [k for d in range(half, 0, -1) for k in sorted({d, n["gy"] - d})] + [0]
    if last > 1:
        @pl.when(jnp.logical_not(at_end))
        def _():
            next_round(last - 2)

    slot_near = slot_plane = 0
    for planes in ((1, 0), (2, 3)):
        if planes[0] == 2:
            pl.semaphore_wait(known_sem.at[last - 1], 2 * len(greeted(last - 1)))
        for k in order:
            for i in planes:
                for core in (1, 0):
                    where = device(gx=i, gy=k, gz=core)
                    if i in above(n["gx"]):
                        row_to(own_row, near_rows, slot_near, near_send, near_recv, where)
                        slot_near += 1
                    elif i == 0 and (k or core):
                        row_to(own_row, plane_rows, slot_plane, plane_send, plane_recv, where)
                        slot_plane += 1
    wait_rows(plane_rows, plane_recv)
    plane_total = folded + jnp.sum(plane_rows[...], axis=0, keepdims=True)
    plane_row[...] = plane_total
    far = beyond(n["gx"])
    for slot, k in enumerate(far):
        row_to(plane_row, far_rows, slot, far_send, far_recv, device(gx=k))
    wait_rows(near_rows, near_recv)
    total = plane_total + jnp.sum(near_rows[...], axis=0, keepdims=True)
    if far:
        wait_rows(far_rows, far_recv)
        total = total + jnp.sum(far_rows[...], axis=0, keepdims=True)
    totals_ref[...] = total
    wait_rows(plane_rows, plane_send)
    wait_rows(near_rows, near_send)
    if far:
        wait_rows(far_rows, far_send)


def above(size):
    return range(1, min(size, 4))


def beyond(size):
    return range(4, size)


def finish(entries, out, totals, residual, tangent, stats, held, sems):
    half = out.shape[0] // 2
    copies = [
        pltpu.make_async_copy(out.at[0:half], residual, sems.at[0]),
        pltpu.make_async_copy(out.at[half:], tangent, sems.at[1]),
    ]
    for copy in copies:
        copy.start()
    row = totals[...]
    first = lax.broadcasted_iota(jnp.int32, row.shape, 1) < row.shape[1] // 2
    squares = jnp.sum(jnp.where(first, row, 0.0), axis=1, keepdims=True) / entries
    curvature = jnp.sum(jnp.where(first, 0.0, row), axis=1, keepdims=True) / entries
    held[0] = jnp.sqrt(squares + root_eps)[0, 0]
    held[1] = curvature[0, 0]
    copies.append(pltpu.make_async_copy(held, stats, sems.at[2]))
    copies[-1].start()
    for copy in copies:
        copy.wait()


def solution(mesh):
    sizes = tuple((axis, mesh.shape[axis]) for axis in ("gx", "gy", "gz"))
    n = dict(sizes)

    def local(fields, macro_strain, material):
        nx, ny, nz = fields.shape[2:]
        lay = Layout(nx, ny, nz)
        consts = [jnp.asarray(m) for m in matrices(lay)]
        hbm = pl.BlockSpec(memory_space=pltpu.HBM)
        vmem = pl.BlockSpec(memory_space=pltpu.VMEM)
        halos = 2 + 2 * nx + 12
        own = lay.own
        plane = n["gy"] * n["gz"]
        near, far = plane * len(above(n["gx"])), len(beyond(n["gx"]))
        dma = pltpu.SemaphoreType.DMA
        out, totals = pl.pallas_call(
            functools.partial(kernel, lay, sizes),
            out_shape=(
                pltpu.VMEM((6 * own, nz), f32),
                pltpu.VMEM((1, nz), f32),
            ),
            in_specs=[hbm] * 8,
            out_specs=(vmem, vmem),
            scratch_shapes=[
                pltpu.VMEM((6, lay.rows, nz), f32),
                pltpu.VMEM((6, lay.rows, nz), f32),
                pltpu.SMEM(macro_strain.shape, f32),
                pltpu.SMEM(material.shape, f32),
                *[pltpu.VMEM(m.shape, bf16) for m in consts],
                pltpu.VMEM((2, 3, 3, lay.points, 256), f32),
                pltpu.VMEM((2, 3, 3, lay.points, 256), f32),
                pltpu.VMEM((2, 2, 6 * own, lay.lanes), bf16),
                pltpu.VMEM((1, nz), f32),
                pltpu.VMEM((1, nz), f32),
                pltpu.VMEM((plane - 1, nz), f32),
                pltpu.VMEM((near, nz), f32),
                pltpu.VMEM((max(far, 1), nz), f32),
                dma,
                dma((7,)),
                dma((halos,)),
                dma((halos,)),
                dma((2,)),
                dma((2,)),
                *[dma] * 6,
                pltpu.SemaphoreType.REGULAR((8,)),
            ],
            compiler_params=pltpu.CompilerParams(
                collective_id=0, has_side_effects=True
            ),
            name="cell",
        )(fields.reshape(6, nx * ny, nz), macro_strain, material, *consts)
        entries = 3.0 * nx * ny * nz * n["gx"] * n["gy"] * n["gz"]
        block = jax.ShapeDtypeStruct((3 * own, nz), f32)
        residual, tangent, stats = pl.pallas_call(
            functools.partial(finish, entries),
            out_shape=(block, block, jax.ShapeDtypeStruct((2,), f32)),
            in_specs=[vmem, vmem],
            out_specs=(hbm, hbm, hbm),
            scratch_shapes=[pltpu.SMEM((2,), f32), dma((3,))],
            compiler_params=pltpu.CompilerParams(vmem_limit_bytes=24 * 2**20),
            name="finish",
        )(out, totals)
        shape = (3, nx, ny, nz)
        return residual.reshape(shape), tangent.reshape(shape), stats

    in_specs = (P("body", None, "gx", "gy", "gz"), P("body", None), P("body"))
    out_specs = (P("body", "gx", "gy", "gz"), P("body", "gx", "gy", "gz"), P("body"))
    return jax.shard_map(local, mesh=mesh, in_specs=in_specs, out_specs=out_specs, check_vma=False)
```

```python
import functools
import math

import jax
import jax.numpy as jnp
import numpy as np
from jax import lax
from jax.experimental import pallas as pl
from jax.experimental.pallas import tpu as pltpu
from jax.sharding import PartitionSpec as P

MESH = pl.DeviceIdType.MESH
spacing = 4.0
root_eps = 1e-06
f32 = jnp.float32
bf16 = jnp.bfloat16


def tables():
    root = math.sqrt(0.6)
    points = np.array([-root, 0.0, root])
    values = np.stack(
        [points * (points - 1.0) / 2.0, 1.0 - points * points, points * (points + 1.0) / 2.0], axis=1
    )
    slopes = np.stack([points - 0.5, -2.0 * points, points + 0.5], axis=1) * (2.0 / spacing)
    weights = np.array([5.0 / 9.0, 8.0 / 9.0, 5.0 / 9.0]) * (spacing / 2.0)
    return values, slopes, weights


def ceil_to(n, m):
    return -(-n // m) * m


class Layout:
    def __init__(self, nx, ny, nz):
        self.nx, self.ny, self.nz = nx, ny, nz
        self.own = nx * ny
        self.xm = self.own
        self.xp = self.xm + 2 * ny
        self.ym_own = self.xp + ny
        self.yp_own = self.ym_own + 2 * nx
        self.corners = self.yp_own + nx
        self.ym_xm = self.corners
        self.ym_xp = self.ym_xm + 4
        self.yp_xm = self.ym_xp + 2
        self.yp_xp = self.yp_xm + 2
        self.used = self.yp_xp + 1
        self.rows = ceil_to(self.used, 16)
        self.ex, self.ey, self.ez = nx // 2 + 1, ny // 2 + 1, nz // 2 + 1
        self.group = ceil_to(self.ex * self.ey, 16)
        self.points = 9 * self.group
        self.lanes = ceil_to(3 * self.ez, 128)

    def row(self, p, r):
        if 0 <= r < self.ny:
            if 0 <= p < self.nx:
                return p * self.ny + r
            if p < 0:
                return self.xm + (p + 2) * self.ny + r
            return self.xp + r
        if r < 0:
            if 0 <= p < self.nx:
                return self.ym_own + 2 * p + r + 2
            if p < 0:
                return self.ym_xm + 2 * (p + 2) + r + 2
            return self.ym_xp + r + 2
        if 0 <= p < self.nx:
            return self.yp_own + p
        if p < 0:
            return self.yp_xm + p + 2
        return self.yp_xp


def split_np(a):
    a = a.astype(np.float32)
    high = np.asarray(a, dtype=jnp.bfloat16)
    low = np.asarray(a - high.astype(np.float32), dtype=jnp.bfloat16)
    return high, low


def matrices(lay):
    values, slopes, weights = tables()
    forward = np.zeros((3, lay.points, lay.rows))
    back = np.zeros((3, lay.own, lay.points))
    pairs = ((slopes, values), (values, slopes), (values, values))
    for kind, (tx, ty) in enumerate(pairs):
        for q1 in range(3):
            for q2 in range(3):
                for ex in range(lay.ex):
                    for ey in range(lay.ey):
                        point = (q1 * 3 + q2) * lay.group + ex * lay.ey + ey
                        for a1 in range(3):
                            for a2 in range(3):
                                p, r = 2 * (ex - 1) + a1, 2 * (ey - 1) + a2
                                factor = tx[q1, a1] * ty[q2, a2]
                                forward[kind, point, lay.row(p, r)] += factor
                                if 0 <= p < lay.nx and 0 <= r < lay.ny:
                                    back[kind, p * lay.ny + r, point] += factor * weights[q1] * weights[q2]
    along_z = np.zeros((2, 2 * lay.nz, lay.lanes))
    z_back = np.zeros((2, lay.lanes, lay.nz))
    inside = [(q3, ez) for q3 in range(3) for ez in range(1, lay.ez - 1)]
    edge = [(q3, ez) for q3 in range(3) for ez in (0, lay.ez - 1)]
    for column, (q3, ez) in enumerate(inside + edge):
        for kind, tz in enumerate((values, slopes)):
            for a3 in range(3):
                z = 2 * (ez - 1) + a3
                if z < 0:
                    k = lay.nz + lay.nz + z
                elif z >= lay.nz:
                    k = lay.nz + z - lay.nz
                else:
                    k = z
                    z_back[kind, column, z] += tz[q3, a3] * weights[q3]
                along_z[kind, k, column] += tz[q3, a3]
    fh, fl = split_np(forward)
    forward = np.concatenate([fh, fh, fl], axis=2).reshape(3 * lay.points, 3 * lay.rows)
    bh, bl = split_np(back)
    back = np.concatenate([bh, bl], axis=1)
    first = np.concatenate(along_z[:, : lay.nz, :128], axis=1)
    second = np.concatenate(along_z[:, :, 128:], axis=1)
    first = np.concatenate(split_np(first), axis=0)
    second = np.stack(split_np(second))
    zh, zl = split_np(z_back)
    z_back = np.concatenate([zh, zl], axis=2)
    return forward, back, first, second, z_back


def split(x):
    high = x.astype(bf16)
    return high, (x - high.astype(f32)).astype(bf16)


def dot(a, b):
    return jnp.dot(a, b, preferred_element_type=f32)


def kernel(
    lay, sizes,
    fields, strain_h, material_h, forward_h, back_h, first_h, second_h, z_back_h,
    out, totals_ref,
    ext, extp, strain, material, forward, back, first, second, z_back, grads, flux, middle,
    own_row, plane_row, plane_rows, near_rows, far_rows,
    load_sem, const_sem, halo_send, halo_recv, core_send, core_recv,
    plane_send, plane_recv, near_send, near_recv, far_send, far_recv, known_sem,
):
    n = dict(sizes)
    me = {axis: lax.axis_index(axis) for axis in ("gx", "gy", "gz")}
    nx, ny, nz = lay.nx, lay.ny, lay.nz
    own, rows = lay.own, lay.rows

    def device(**shifts):
        return {
            axis: lax.rem(me[axis] + (shift % n[axis]), n[axis]) for axis, shift in shifts.items()
        }

    load = pltpu.make_async_copy(fields, ext.at[:, 0:own, :], load_sem)
    load.start()

    barrier = pltpu.get_barrier_semaphore()
    around = [(1, 1), (1, -1), (-1, 1), (-1, -1), (1, 0), (-1, 0), (0, 1), (0, -1)]
    near = [device(gx=i, gy=j) for i, j in around] + [device(gz=1)]
    near += [device(gx=i, gy=j, gz=1) for i, j in around]
    for where in near:
        pl.semaphore_signal(barrier, inc=1, device_id=where, device_id_type=MESH)

    constants = [
        pltpu.make_async_copy(source, target, const_sem.at[i])
        for i, (source, target) in enumerate(
            (
                (first_h, first), (forward_h, forward), (second_h, second), (back_h, back),
                (z_back_h, z_back), (strain_h, strain), (material_h, material),
            )
        )
    ]
    for copy in constants:
        copy.start()
    if rows > lay.used:
        for target in (ext, extp):
            target[:, lay.used :, :] = jnp.zeros((6, rows - lay.used, nz), f32)

    def along_first(nodes):
        high, low = split(nodes)
        weights = first[0:nz]
        return dot(
            jnp.concatenate([high, low], axis=1), jnp.concatenate([weights, weights], axis=0)
        ) + dot(high, first[nz:])

    def along_second(mine, other):
        high, low = split(jnp.concatenate([mine, other], axis=1))
        return dot(high, second[0]) + dot(low, second[0]) + dot(high, second[1])

    count = [0]
    sends = []

    def send(source, target, where, into=ext):
        i = count[0]
        count[0] += 1
        copy = pltpu.make_async_remote_copy(
            src_ref=ext.at[:, source[0] : source[0] + source[1], :],
            dst_ref=into.at[:, target : target + source[1], :],
            send_sem=halo_send.at[i],
            recv_sem=halo_recv.at[i],
            device_id=where,
            device_id_type=MESH,
        )
        copy.start()
        sends.append(copy)

    load.wait()
    pl.semaphore_wait(barrier, len(near))
    for core, into in enumerate((ext, extp)):
        for p in range(2):
            start = (nx - 2 + p) * ny
            send((start + ny - 2, 2), lay.ym_xm + 2 * p, device(gx=1, gy=1, gz=core), into)
            send((start, 1), lay.yp_xm + p, device(gx=1, gy=-1, gz=core), into)
        send((ny - 2, 2), lay.ym_xp, device(gx=-1, gy=1, gz=core), into)
        send((0, 1), lay.yp_xp, device(gx=-1, gy=-1, gz=core), into)
    send(((nx - 2) * ny, 2 * ny), lay.xm, device(gx=1))
    send((0, ny), lay.xp, device(gx=-1))
    for p in range(nx):
        send((p * ny + ny - 2, 2), lay.ym_own + 2 * p, device(gy=1))
        send((p * ny, 1), lay.yp_own + p, device(gy=-1))

    def to_core(i, start, stop):
        return pltpu.make_async_remote_copy(
            src_ref=ext.at[:, start:stop, :],
            dst_ref=extp.at[:, start:stop, :],
            send_sem=core_send.at[i],
            recv_sem=core_recv.at[i],
            device_id=device(gz=1),
            device_id_type=MESH,
        )

    core_own = to_core(0, 0, own)
    core_own.start()

    rounds = {
        "gx": max(1, math.ceil(math.log2(n["gx"] / 2))), "gy": max(1, math.ceil(math.log2(n["gy"] / 2)))
    }
    last = max(rounds.values())

    def greeted(step):
        shifts = [(axis, 2**step) for axis in ("gx", "gy") if step < rounds[axis]]
        if step == last - 1 and step:
            shifts.append(("gx", 2 ** (step - 1)))
        return shifts

    def greet(step):
        for axis, d in greeted(step):
            for shift in (d, -d):
                pl.semaphore_signal(
                    known_sem.at[step], inc=1, device_id=device(**{axis: shift}), device_id_type=MESH
                )

    def next_round(step):
        pl.semaphore_wait(known_sem.at[step], 2 * len(greeted(step)))
        greet(step + 1)

    here, top = me["gx"], n["gx"] - 1
    at_end = (here >= top - 2) | (here <= 1)
    greet(0)
    for step in range(last - 2):
        next_round(step)
    if last > 1:
        @pl.when(at_end)
        def _():
            next_round(last - 2)

    for copy in constants:
        copy.wait()
    late = lay.corners // 16 * 16
    bounds = [0, own, late, rows]
    sizes_of = [stop - start for start, stop in zip(bounds, bounds[1:])]

    def nodes(ref, i):
        return ref[:, bounds[i] : bounds[i + 1]].reshape(6 * sizes_of[i], nz)

    z_first = [along_first(nodes(ext, 0))]
    core_own.wait()
    z_second = [along_second(nodes(ext, 0), nodes(extp, 0))]
    for copy in sends[12:]:
        copy.wait()
    core_halo = to_core(1, own, lay.corners)
    core_halo.start()
    z_first.append(along_first(nodes(ext, 1)))
    for copy in sends[:12]:
        copy.wait()

    def to_points(tile, pieces):
        parts_of = [split(z) for z in pieces]

        def one(pair):
            parts = []
            for kind in range(2):
                sides = []
                lanes = slice(kind * 128, kind * 128 + 128)
                for c in (2 * pair, 2 * pair + 1):
                    high, low = (
                        jnp.concatenate(
                            [
                                part[hl][c * size : c * size + size, lanes]
                                for part, size in zip(parts_of, sizes_of)
                            ],
                            axis=0,
                        )
                        for hl in range(2)
                    )
                    sides.append(jnp.concatenate([high, low, high], axis=0))
                parts.append(jnp.concatenate(sides, axis=1))
            both = dot(forward[: 2 * lay.points], parts[0])
            grads[tile, pair, 0] = both[: lay.points]
            grads[tile, pair, 1] = both[lay.points :]
            grads[tile, pair, 2] = dot(forward[2 * lay.points :], parts[1])

        return one

    shear, lame = material[0], material[1]
    ratio = lame / shear
    shift = [
        [strain[i, j] + (1.0 if i == j else 0.0) for j in range(3)] for i in range(3)
    ]

    def side(c):
        return slice((c % 2) * 128, (c % 2) * 128 + 128)

    def stresses(tile):
        def points(i, carry):
            for half in range(2):
                if isinstance(i, int):
                    block = slice(i * 16 + half * 8, i * 16 + half * 8 + 8)
                else:
                    block = pl.ds(pl.multiple_of(i * 16 + half * 8, 8), 8)

                def gradient(c, along):
                    return grads[tile, c // 2, along, block, side(c)]

                f = [[gradient(r, c) + shift[r][c] for c in range(3)] for r in range(3)]
                dv = [[gradient(3 + r, c) for c in range(3)] for r in range(3)]
                cof = [
                    [
                        f[(r + 1) % 3][(c + 1) % 3] * f[(r + 2) % 3][(c + 2) % 3]
                        - f[(r + 1) % 3][(c + 2) % 3] * f[(r + 2) % 3][(c + 1) % 3]
                        for c in range(3)
                    ]
                    for r in range(3)
                ]
                det = f[0][0] * cof[0][0] + f[0][1] * cof[0][1] + f[0][2] * cof[0][2]
                inverse = 1.0 / det
                g = [[cof[r][c] * inverse for c in range(3)] for r in range(3)]
                pressure = ratio * jnp.log(det) - 1.0
                soft = -pressure
                for r in range(3):
                    for c in range(3):
                        flux[tile, r // 2, c, block, side(r)] = f[r][c] + pressure * g[r][c]
                m = [
                    [
                        g[r][0] * dv[c][0] + g[r][1] * dv[c][1] + g[r][2] * dv[c][2]
                        for c in range(3)
                    ]
                    for r in range(3)
                ]
                trace = ratio * (m[0][0] + m[1][1] + m[2][2])
                w = [
                    [trace + soft * m[r][c] if r == c else soft * m[r][c] for c in range(3)]
                    for r in range(3)
                ]
                for r in range(3):
                    for c in range(3):
                        flux[tile, (3 + r) // 2, c, block, side(3 + r)] = dv[r][c] + (
                            w[r][0] * g[0][c] + w[r][1] * g[1][c] + w[r][2] * g[2][c]
                        )
            return carry

        return points

    def back_pair(tile, pair):
        def plane(kind, along):
            high, low = split(flux[tile, pair, along])
            both = dot(back[kind], high)
            return both[:own] + both[own:] + dot(back[kind, :own], low)

        for kind, part in enumerate((plane(0, 0) + plane(1, 1), plane(2, 2))):
            for hl, piece in enumerate(split(part)):
                for c in (2 * pair, 2 * pair + 1):
                    at = slice(c * own, c * own + own)
                    middle[kind, hl, at, tile * 128 : tile * 128 + 128] = piece[:, side(c)]

    z_first.append(along_first(nodes(ext, 2)))
    points_of = to_points(0, z_first)
    for pair in range(3):
        points_of(pair)
    blocks = lay.points // 16
    for i in range(blocks):
        stresses(0)(i, 0)
    core_halo.wait()
    z_second += [along_second(nodes(ext, i), nodes(extp, i)) for i in (1, 2)]
    points_of = to_points(1, z_second)
    for pair in range(3):
        points_of(pair)
    for i in range(blocks):
        if i % (blocks // 3) == 0:
            back_pair(0, i // (blocks // 3))
        stresses(1)(i, 0)
    for pair in range(3):
        back_pair(1, pair)
    result = dot(middle[0, 1], z_back[0, :, :nz]) + dot(middle[1, 1], z_back[1, :, :nz])
    both = dot(middle[0, 0], z_back[0]) + dot(middle[1, 0], z_back[1])
    result = (result + both[:, :nz] + both[:, nz:]) * shear
    out[...] = result
    sums = []
    for c0 in (0, 3):
        total = jnp.zeros((8, nz), f32)
        for c in range(c0, c0 + 3):
            part = result[c * own : c * own + own]
            product = part * (part if c < 3 else ext[c, :own])
            for k in range(own // 8):
                total = total + product[8 * k : 8 * k + 8]
        sums.append(total + pltpu.roll(total, nz // 2, 1))
    lane = lax.broadcasted_iota(jnp.int32, (8, nz), 1)
    folded = jnp.sum(jnp.where(lane < nz // 2, sums[0], sums[1]), axis=0, keepdims=True)
    own_row[...] = folded

    def row_to(source, target, slot, send_sem, recv_sem, where):
        pltpu.make_async_remote_copy(
            src_ref=source,
            dst_ref=target.at[slot : slot + 1],
            send_sem=send_sem,
            recv_sem=recv_sem,
            device_id=where,
            device_id_type=MESH,
        ).start()

    def wait_rows(rows, sem):
        pltpu.make_async_copy(rows, rows, sem).wait()

    half = n["gy"] // 2
    order = [k for d in range(half, 0, -1) for k in sorted({d, n["gy"] - d})] + [0]
    if last > 1:
        @pl.when(jnp.logical_not(at_end))
        def _():
            next_round(last - 2)

    slot_near = slot_plane = 0
    for planes in ((1, 0), (2, 3)):
        if planes[0] == 2:
            pl.semaphore_wait(known_sem.at[last - 1], 2 * len(greeted(last - 1)))
        for k in order:
            for i in planes:
                for core in (1, 0):
                    where = device(gx=i, gy=k, gz=core)
                    if i in above(n["gx"]):
                        row_to(own_row, near_rows, slot_near, near_send, near_recv, where)
                        slot_near += 1
                    elif i == 0 and (k or core):
                        row_to(own_row, plane_rows, slot_plane, plane_send, plane_recv, where)
                        slot_plane += 1
    wait_rows(plane_rows, plane_recv)
    plane_total = folded + jnp.sum(plane_rows[...], axis=0, keepdims=True)
    plane_row[...] = plane_total
    far = beyond(n["gx"])
    for slot, k in enumerate(far):
        row_to(plane_row, far_rows, slot, far_send, far_recv, device(gx=k))
    wait_rows(near_rows, near_recv)
    total = plane_total + jnp.sum(near_rows[...], axis=0, keepdims=True)
    if far:
        wait_rows(far_rows, far_recv)
        total = total + jnp.sum(far_rows[...], axis=0, keepdims=True)
    totals_ref[...] = total
    wait_rows(plane_rows, plane_send)
    wait_rows(near_rows, near_send)
    if far:
        wait_rows(far_rows, far_send)


def above(size):
    return range(1, min(size, 4))


def beyond(size):
    return range(4, size)


def finish(entries, out, totals, residual, tangent, stats, held, sems):
    half = out.shape[0] // 2
    copies = [
        pltpu.make_async_copy(out.at[0:half], residual, sems.at[0]),
        pltpu.make_async_copy(out.at[half:], tangent, sems.at[1]),
    ]
    for copy in copies:
        copy.start()
    row = totals[...]
    first = lax.broadcasted_iota(jnp.int32, row.shape, 1) < row.shape[1] // 2
    squares = jnp.sum(jnp.where(first, row, 0.0), axis=1, keepdims=True) / entries
    curvature = jnp.sum(jnp.where(first, 0.0, row), axis=1, keepdims=True) / entries
    held[0] = jnp.sqrt(squares + root_eps)[0, 0]
    held[1] = curvature[0, 0]
    copies.append(pltpu.make_async_copy(held, stats, sems.at[2]))
    copies[-1].start()
    for copy in copies:
        copy.wait()


def solution(mesh):
    sizes = tuple((axis, mesh.shape[axis]) for axis in ("gx", "gy", "gz"))
    n = dict(sizes)

    def local(fields, macro_strain, material):
        nx, ny, nz = fields.shape[2:]
        lay = Layout(nx, ny, nz)
        consts = [jnp.asarray(m) for m in matrices(lay)]
        hbm = pl.BlockSpec(memory_space=pltpu.HBM)
        vmem = pl.BlockSpec(memory_space=pltpu.VMEM)
        halos = 2 + 2 * nx + 12
        own = lay.own
        plane = n["gy"] * n["gz"]
        near, far = plane * len(above(n["gx"])), len(beyond(n["gx"]))
        dma = pltpu.SemaphoreType.DMA
        out, totals = pl.pallas_call(
            functools.partial(kernel, lay, sizes),
            out_shape=(
                pltpu.VMEM((6 * own, nz), f32),
                pltpu.VMEM((1, nz), f32),
            ),
            in_specs=[hbm] * 8,
            out_specs=(vmem, vmem),
            scratch_shapes=[
                pltpu.VMEM((6, lay.rows, nz), f32),
                pltpu.VMEM((6, lay.rows, nz), f32),
                pltpu.SMEM(macro_strain.shape, f32),
                pltpu.SMEM(material.shape, f32),
                *[pltpu.VMEM(m.shape, bf16) for m in consts],
                pltpu.VMEM((2, 3, 3, lay.points, 256), f32),
                pltpu.VMEM((2, 3, 3, lay.points, 256), f32),
                pltpu.VMEM((2, 2, 6 * own, lay.lanes), bf16),
                pltpu.VMEM((1, nz), f32),
                pltpu.VMEM((1, nz), f32),
                pltpu.VMEM((plane - 1, nz), f32),
                pltpu.VMEM((near, nz), f32),
                pltpu.VMEM((max(far, 1), nz), f32),
                dma,
                dma((7,)),
                dma((halos,)),
                dma((halos,)),
                dma((2,)),
                dma((2,)),
                *[dma] * 6,
                pltpu.SemaphoreType.REGULAR((8,)),
            ],
            compiler_params=pltpu.CompilerParams(
                collective_id=0, has_side_effects=True
            ),
            name="cell",
        )(fields.reshape(6, nx * ny, nz), macro_strain, material, *consts)
        entries = 3.0 * nx * ny * nz * n["gx"] * n["gy"] * n["gz"]
        block = jax.ShapeDtypeStruct((3 * own, nz), f32)
        residual, tangent, stats = pl.pallas_call(
            functools.partial(finish, entries),
            out_shape=(block, block, jax.ShapeDtypeStruct((2,), f32)),
            in_specs=[vmem, vmem],
            out_specs=(hbm, hbm, hbm),
            scratch_shapes=[pltpu.SMEM((2,), f32), dma((3,))],
            compiler_params=pltpu.CompilerParams(vmem_limit_bytes=24 * 2**20),
            name="finish",
        )(out, totals)
        shape = (3, nx, ny, nz)
        return residual.reshape(shape), tangent.reshape(shape), stats

    in_specs = (P("body", None, "gx", "gy", "gz"), P("body", None), P("body"))
    out_specs = (P("body", "gx", "gy", "gz"), P("body", "gx", "gy", "gz"), P("body"))
    return jax.shard_map(local, mesh=mesh, in_specs=in_specs, out_specs=out_specs, check_vma=False)
```

```python
import functools
import math

import jax
import jax.numpy as jnp
import numpy as np
from jax import lax
from jax.experimental import pallas as pl
from jax.experimental.pallas import tpu as pltpu
from jax.sharding import PartitionSpec as P

MESH = pl.DeviceIdType.MESH
spacing = 4.0
root_eps = 1e-06
f32 = jnp.float32
bf16 = jnp.bfloat16


def tables():
    root = math.sqrt(0.6)
    points = np.array([-root, 0.0, root])
    values = np.stack(
        [points * (points - 1.0) / 2.0, 1.0 - points * points, points * (points + 1.0) / 2.0], axis=1
    )
    slopes = np.stack([points - 0.5, -2.0 * points, points + 0.5], axis=1) * (2.0 / spacing)
    weights = np.array([5.0 / 9.0, 8.0 / 9.0, 5.0 / 9.0]) * (spacing / 2.0)
    return values, slopes, weights


def ceil_to(n, m):
    return -(-n // m) * m


class Layout:
    def __init__(self, nx, ny, nz):
        self.nx, self.ny, self.nz = nx, ny, nz
        self.own = nx * ny
        self.xm = self.own
        self.xp = self.xm + 2 * ny
        self.ym_own = self.xp + ny
        self.yp_own = self.ym_own + 2 * nx
        self.corners = self.yp_own + nx
        self.ym_xm = self.corners
        self.ym_xp = self.ym_xm + 4
        self.yp_xm = self.ym_xp + 2
        self.yp_xp = self.yp_xm + 2
        self.used = self.yp_xp + 1
        self.rows = ceil_to(self.used, 16)
        self.ex, self.ey, self.ez = nx // 2 + 1, ny // 2 + 1, nz // 2 + 1
        self.group = ceil_to(self.ex * self.ey, 16)
        self.points = 9 * self.group
        self.lanes = ceil_to(3 * self.ez, 128)

    def row(self, p, r):
        if 0 <= r < self.ny:
            if 0 <= p < self.nx:
                return p * self.ny + r
            if p < 0:
                return self.xm + (p + 2) * self.ny + r
            return self.xp + r
        if r < 0:
            if 0 <= p < self.nx:
                return self.ym_own + 2 * p + r + 2
            if p < 0:
                return self.ym_xm + 2 * (p + 2) + r + 2
            return self.ym_xp + r + 2
        if 0 <= p < self.nx:
            return self.yp_own + p
        if p < 0:
            return self.yp_xm + p + 2
        return self.yp_xp


def split_np(a):
    a = a.astype(np.float32)
    high = np.asarray(a, dtype=jnp.bfloat16)
    low = np.asarray(a - high.astype(np.float32), dtype=jnp.bfloat16)
    return high, low


def matrices(lay):
    values, slopes, weights = tables()
    forward = np.zeros((3, lay.points, lay.rows))
    back = np.zeros((3, lay.own, lay.points))
    pairs = ((slopes, values), (values, slopes), (values, values))
    for kind, (tx, ty) in enumerate(pairs):
        for q1 in range(3):
            for q2 in range(3):
                for ex in range(lay.ex):
                    for ey in range(lay.ey):
                        point = (q1 * 3 + q2) * lay.group + ex * lay.ey + ey
                        for a1 in range(3):
                            for a2 in range(3):
                                p, r = 2 * (ex - 1) + a1, 2 * (ey - 1) + a2
                                factor = tx[q1, a1] * ty[q2, a2]
                                forward[kind, point, lay.row(p, r)] += factor
                                if 0 <= p < lay.nx and 0 <= r < lay.ny:
                                    back[kind, p * lay.ny + r, point] += factor * weights[q1] * weights[q2]
    along_z = np.zeros((2, 2 * lay.nz, lay.lanes))
    z_back = np.zeros((2, lay.lanes, lay.nz))
    inside = [(q3, ez) for q3 in range(3) for ez in range(1, lay.ez - 1)]
    edge = [(q3, ez) for q3 in range(3) for ez in (0, lay.ez - 1)]
    for column, (q3, ez) in enumerate(inside + edge):
        for kind, tz in enumerate((values, slopes)):
            for a3 in range(3):
                z = 2 * (ez - 1) + a3
                if z < 0:
                    k = lay.nz + lay.nz + z
                elif z >= lay.nz:
                    k = lay.nz + z - lay.nz
                else:
                    k = z
                    z_back[kind, column, z] += tz[q3, a3] * weights[q3]
                along_z[kind, k, column] += tz[q3, a3]
    fh, fl = split_np(forward)
    forward = np.concatenate([fh, fh, fl], axis=2).reshape(3 * lay.points, 3 * lay.rows)
    bh, bl = split_np(back)
    back = np.concatenate([bh, bl], axis=1)
    first = np.concatenate(along_z[:, : lay.nz, :128], axis=1)
    second = np.concatenate(along_z[:, :, 128:], axis=1)
    first = np.concatenate(split_np(first), axis=0)
    second = np.stack(split_np(second))
    zh, zl = split_np(z_back)
    z_back = np.concatenate([zh, zl], axis=2)
    return forward, back, first, second, z_back


def split(x):
    high = x.astype(bf16)
    return high, (x - high.astype(f32)).astype(bf16)


def dot(a, b):
    return jnp.dot(a, b, preferred_element_type=f32)


def kernel(
    lay, sizes,
    fields, strain_h, material_h, forward_h, back_h, first_h, second_h, z_back_h,
    out, totals_ref,
    ext, extp, strain, material, forward, back, first, second, z_back, grads, flux, middle,
    own_row, plane_row, plane_rows, near_rows, far_rows,
    load_sem, const_sem, halo_send, halo_recv, core_send, core_recv,
    plane_send, plane_recv, near_send, near_recv, far_send, far_recv, known_sem,
):
    n = dict(sizes)
    me = {axis: lax.axis_index(axis) for axis in ("gx", "gy", "gz")}
    nx, ny, nz = lay.nx, lay.ny, lay.nz
    own, rows = lay.own, lay.rows

    def device(**shifts):
        return {
            axis: lax.rem(me[axis] + (shift % n[axis]), n[axis]) for axis, shift in shifts.items()
        }

    load = pltpu.make_async_copy(fields, ext.at[:, 0:own, :], load_sem)
    load.start()

    barrier = pltpu.get_barrier_semaphore()
    beside = [(i, j) for i in (-1, 1) for j in (1, -1, 0)]
    near = [device(gx=i, gy=j, gz=core) for i, j in beside for core in (0, 1)]
    near += [device(gy=j, gz=core) for j in (1, -1) for core in (0, 1)] + [device(gz=1)]
    for where in near:
        pl.semaphore_signal(barrier, inc=1, device_id=where, device_id_type=MESH)

    constants = [
        pltpu.make_async_copy(source, target, const_sem.at[i])
        for i, (source, target) in enumerate(
            (
                (first_h, first), (forward_h, forward), (second_h, second), (back_h, back),
                (z_back_h, z_back), (strain_h, strain), (material_h, material),
            )
        )
    ]
    for copy in constants:
        copy.start()
    if rows > lay.used:
        for target in (ext, extp):
            target[:, lay.used :, :] = jnp.zeros((6, rows - lay.used, nz), f32)

    def along_first(nodes):
        high, low = split(nodes)
        weights = first[0:nz]
        return dot(
            jnp.concatenate([high, low], axis=1), jnp.concatenate([weights, weights], axis=0)
        ) + dot(high, first[nz:])

    def along_second(mine, other):
        high, low = split(jnp.concatenate([mine, other], axis=1))
        return dot(high, second[0]) + dot(low, second[0]) + dot(high, second[1])

    count = [0]
    sends = []

    def send(source, target, where, into=ext):
        i = count[0]
        count[0] += 1
        copy = pltpu.make_async_remote_copy(
            src_ref=ext.at[:, source[0] : source[0] + source[1], :],
            dst_ref=into.at[:, target : target + source[1], :],
            send_sem=halo_send.at[i],
            recv_sem=halo_recv.at[i],
            device_id=where,
            device_id_type=MESH,
        )
        copy.start()
        sends.append(copy)

    load.wait()
    pl.semaphore_wait(barrier, len(near))
    for core, into in enumerate((ext, extp)):
        for p in range(2):
            start = (nx - 2 + p) * ny
            send((start + ny - 2, 2), lay.ym_xm + 2 * p, device(gx=1, gy=1, gz=core), into)
            send((start, 1), lay.yp_xm + p, device(gx=1, gy=-1, gz=core), into)
    send(((nx - 2) * ny, 2 * ny), lay.xm, device(gx=1))
    for core, into in enumerate((ext, extp)):
        send((ny - 2, 2), lay.ym_xp, device(gx=-1, gy=1, gz=core), into)
        send((0, 1), lay.yp_xp, device(gx=-1, gy=-1, gz=core), into)
    send((0, ny), lay.xp, device(gx=-1))
    for p in range(nx):
        send((p * ny + ny - 2, 2), lay.ym_own + 2 * p, device(gy=1))
        send((p * ny, 1), lay.yp_own + p, device(gy=-1))

    def to_core(i, start, stop):
        return pltpu.make_async_remote_copy(
            src_ref=ext.at[:, start:stop, :],
            dst_ref=extp.at[:, start:stop, :],
            send_sem=core_send.at[i],
            recv_sem=core_recv.at[i],
            device_id=device(gz=1),
            device_id_type=MESH,
        )

    core_own = to_core(0, 0, own)
    core_own.start()

    rounds = {
        "gx": max(1, math.ceil(math.log2(n["gx"] / 2))), "gy": max(1, math.ceil(math.log2(n["gy"] / 2)))
    }
    last = max(rounds.values())

    def greeted(step):
        shifts = [(axis, 2**step) for axis in ("gx", "gy") if step < rounds[axis]]
        if step == last - 1 and step:
            shifts.append(("gx", 2 ** (step - 1)))
        return shifts

    def greet(step):
        for axis, d in greeted(step):
            for shift in (d, -d):
                pl.semaphore_signal(
                    known_sem.at[step], inc=1, device_id=device(**{axis: shift}), device_id_type=MESH
                )

    def next_round(step):
        pl.semaphore_wait(known_sem.at[step], 2 * len(greeted(step)))
        greet(step + 1)

    here, top = me["gx"], n["gx"] - 1
    at_end = (here >= top - 2) | (here <= 1)
    greet(0)
    for step in range(last - 2):
        next_round(step)
    if last > 1:
        @pl.when(at_end)
        def _():
            next_round(last - 2)

    for copy in constants:
        copy.wait()
    late = lay.corners // 16 * 16
    bounds = [0, own, late, rows]
    sizes_of = [stop - start for start, stop in zip(bounds, bounds[1:])]

    def nodes(ref, i):
        return ref[:, bounds[i] : bounds[i + 1]].reshape(6 * sizes_of[i], nz)

    z_first = [along_first(nodes(ext, 0))]
    core_own.wait()
    z_second = [along_second(nodes(ext, 0), nodes(extp, 0))]
    for copy in sends[8:9] + sends[13:]:
        copy.wait()
    core_halo = to_core(1, own, lay.corners)
    core_halo.start()
    z_first.append(along_first(nodes(ext, 1)))
    for copy in sends[:8] + sends[9:13]:
        copy.wait()

    def to_points(tile, pieces):
        parts_of = [split(z) for z in pieces]

        def one(pair):
            parts = []
            for kind in range(2):
                sides = []
                lanes = slice(kind * 128, kind * 128 + 128)
                for c in (2 * pair, 2 * pair + 1):
                    high, low = (
                        jnp.concatenate(
                            [
                                part[hl][c * size : c * size + size, lanes]
                                for part, size in zip(parts_of, sizes_of)
                            ],
                            axis=0,
                        )
                        for hl in range(2)
                    )
                    sides.append(jnp.concatenate([high, low, high], axis=0))
                parts.append(jnp.concatenate(sides, axis=1))
            both = dot(forward[: 2 * lay.points], parts[0])
            grads[tile, pair, 0] = both[: lay.points]
            grads[tile, pair, 1] = both[lay.points :]
            grads[tile, pair, 2] = dot(forward[2 * lay.points :], parts[1])

        return one

    shear, lame = material[0], material[1]
    ratio = lame / shear
    shift = [
        [strain[i, j] + (1.0 if i == j else 0.0) for j in range(3)] for i in range(3)
    ]

    def side(c):
        return slice((c % 2) * 128, (c % 2) * 128 + 128)

    def stresses(tile):
        def points(i, carry):
            for half in range(2):
                if isinstance(i, int):
                    block = slice(i * 16 + half * 8, i * 16 + half * 8 + 8)
                else:
                    block = pl.ds(pl.multiple_of(i * 16 + half * 8, 8), 8)

                def gradient(c, along):
                    return grads[tile, c // 2, along, block, side(c)]

                f = [[gradient(r, c) + shift[r][c] for c in range(3)] for r in range(3)]
                dv = [[gradient(3 + r, c) for c in range(3)] for r in range(3)]
                cof = [
                    [
                        f[(r + 1) % 3][(c + 1) % 3] * f[(r + 2) % 3][(c + 2) % 3]
                        - f[(r + 1) % 3][(c + 2) % 3] * f[(r + 2) % 3][(c + 1) % 3]
                        for c in range(3)
                    ]
                    for r in range(3)
                ]
                det = f[0][0] * cof[0][0] + f[0][1] * cof[0][1] + f[0][2] * cof[0][2]
                inverse = 1.0 / det
                g = [[cof[r][c] * inverse for c in range(3)] for r in range(3)]
                pressure = ratio * jnp.log(det) - 1.0
                soft = -pressure
                for r in range(3):
                    for c in range(3):
                        flux[tile, r // 2, c, block, side(r)] = f[r][c] + pressure * g[r][c]
                m = [
                    [
                        g[r][0] * dv[c][0] + g[r][1] * dv[c][1] + g[r][2] * dv[c][2]
                        for c in range(3)
                    ]
                    for r in range(3)
                ]
                trace = ratio * (m[0][0] + m[1][1] + m[2][2])
                w = [
                    [trace + soft * m[r][c] if r == c else soft * m[r][c] for c in range(3)]
                    for r in range(3)
                ]
                for r in range(3):
                    for c in range(3):
                        flux[tile, (3 + r) // 2, c, block, side(3 + r)] = dv[r][c] + (
                            w[r][0] * g[0][c] + w[r][1] * g[1][c] + w[r][2] * g[2][c]
                        )
            return carry

        return points

    def back_pair(tile, pair):
        def plane(kind, along):
            high, low = split(flux[tile, pair, along])
            both = dot(back[kind], high)
            return both[:own] + both[own:] + dot(back[kind, :own], low)

        for kind, part in enumerate((plane(0, 0) + plane(1, 1), plane(2, 2))):
            for hl, piece in enumerate(split(part)):
                for c in (2 * pair, 2 * pair + 1):
                    at = slice(c * own, c * own + own)
                    middle[kind, hl, at, tile * 128 : tile * 128 + 128] = piece[:, side(c)]

    z_first.append(along_first(nodes(ext, 2)))
    points_of = to_points(0, z_first)
    for pair in range(3):
        points_of(pair)
    blocks = lay.points // 16
    for i in range(blocks):
        stresses(0)(i, 0)
    core_halo.wait()
    z_second += [along_second(nodes(ext, i), nodes(extp, i)) for i in (1, 2)]
    points_of = to_points(1, z_second)
    for pair in range(3):
        points_of(pair)
    for i in range(blocks):
        if i % (blocks // 3) == 0:
            back_pair(0, i // (blocks // 3))
        stresses(1)(i, 0)
    for pair in range(3):
        back_pair(1, pair)
    result = dot(middle[0, 1], z_back[0, :, :nz]) + dot(middle[1, 1], z_back[1, :, :nz])
    both = dot(middle[0, 0], z_back[0]) + dot(middle[1, 0], z_back[1])
    result = (result + both[:, :nz] + both[:, nz:]) * shear
    out[...] = result
    sums = []
    for c0 in (0, 3):
        total = jnp.zeros((8, nz), f32)
        for c in range(c0, c0 + 3):
            part = result[c * own : c * own + own]
            product = part * (part if c < 3 else ext[c, :own])
            for k in range(own // 8):
                total = total + product[8 * k : 8 * k + 8]
        sums.append(total + pltpu.roll(total, nz // 2, 1))
    lane = lax.broadcasted_iota(jnp.int32, (8, nz), 1)
    folded = jnp.sum(jnp.where(lane < nz // 2, sums[0], sums[1]), axis=0, keepdims=True)
    own_row[...] = folded

    def row_to(source, target, slot, send_sem, recv_sem, where):
        pltpu.make_async_remote_copy(
            src_ref=source,
            dst_ref=target.at[slot : slot + 1],
            send_sem=send_sem,
            recv_sem=recv_sem,
            device_id=where,
            device_id_type=MESH,
        ).start()

    def wait_rows(rows, sem):
        pltpu.make_async_copy(rows, rows, sem).wait()

    half = n["gy"] // 2
    order = [k for d in range(half, 0, -1) for k in sorted({d, n["gy"] - d})] + [0]
    if last > 1:
        @pl.when(jnp.logical_not(at_end))
        def _():
            next_round(last - 2)

    slot_near = slot_plane = 0
    for planes in ((1, 0), (2, 3)):
        if planes[0] == 2:
            pl.semaphore_wait(known_sem.at[last - 1], 2 * len(greeted(last - 1)))
        for k in order:
            for i in planes:
                for core in (1, 0):
                    where = device(gx=i, gy=k, gz=core)
                    if i in above(n["gx"]):
                        row_to(own_row, near_rows, slot_near, near_send, near_recv, where)
                        slot_near += 1
                    elif i == 0 and (k or core):
                        row_to(own_row, plane_rows, slot_plane, plane_send, plane_recv, where)
                        slot_plane += 1
    wait_rows(plane_rows, plane_recv)
    plane_total = folded + jnp.sum(plane_rows[...], axis=0, keepdims=True)
    plane_row[...] = plane_total
    far = beyond(n["gx"])
    for slot, k in enumerate(far):
        row_to(plane_row, far_rows, slot, far_send, far_recv, device(gx=k))
    wait_rows(near_rows, near_recv)
    total = plane_total + jnp.sum(near_rows[...], axis=0, keepdims=True)
    if far:
        wait_rows(far_rows, far_recv)
        total = total + jnp.sum(far_rows[...], axis=0, keepdims=True)
    totals_ref[...] = total
    wait_rows(plane_rows, plane_send)
    wait_rows(near_rows, near_send)
    if far:
        wait_rows(far_rows, far_send)


def above(size):
    return range(1, min(size, 4))


def beyond(size):
    return range(4, size)


def finish(entries, out, totals, residual, tangent, stats, held, sems):
    half = out.shape[0] // 2
    copies = [
        pltpu.make_async_copy(out.at[0:half], residual, sems.at[0]),
        pltpu.make_async_copy(out.at[half:], tangent, sems.at[1]),
    ]
    for copy in copies:
        copy.start()
    row = totals[...]
    first = lax.broadcasted_iota(jnp.int32, row.shape, 1) < row.shape[1] // 2
    squares = jnp.sum(jnp.where(first, row, 0.0), axis=1, keepdims=True) / entries
    curvature = jnp.sum(jnp.where(first, 0.0, row), axis=1, keepdims=True) / entries
    held[0] = jnp.sqrt(squares + root_eps)[0, 0]
    held[1] = curvature[0, 0]
    copies.append(pltpu.make_async_copy(held, stats, sems.at[2]))
    copies[-1].start()
    for copy in copies:
        copy.wait()


def solution(mesh):
    sizes = tuple((axis, mesh.shape[axis]) for axis in ("gx", "gy", "gz"))
    n = dict(sizes)

    def local(fields, macro_strain, material):
        nx, ny, nz = fields.shape[2:]
        lay = Layout(nx, ny, nz)
        consts = [jnp.asarray(m) for m in matrices(lay)]
        hbm = pl.BlockSpec(memory_space=pltpu.HBM)
        vmem = pl.BlockSpec(memory_space=pltpu.VMEM)
        halos = 2 + 2 * nx + 12
        own = lay.own
        plane = n["gy"] * n["gz"]
        near, far = plane * len(above(n["gx"])), len(beyond(n["gx"]))
        dma = pltpu.SemaphoreType.DMA
        out, totals = pl.pallas_call(
            functools.partial(kernel, lay, sizes),
            out_shape=(
                pltpu.VMEM((6 * own, nz), f32),
                pltpu.VMEM((1, nz), f32),
            ),
            in_specs=[hbm] * 8,
            out_specs=(vmem, vmem),
            scratch_shapes=[
                pltpu.VMEM((6, lay.rows, nz), f32),
                pltpu.VMEM((6, lay.rows, nz), f32),
                pltpu.SMEM(macro_strain.shape, f32),
                pltpu.SMEM(material.shape, f32),
                *[pltpu.VMEM(m.shape, bf16) for m in consts],
                pltpu.VMEM((2, 3, 3, lay.points, 256), f32),
                pltpu.VMEM((2, 3, 3, lay.points, 256), f32),
                pltpu.VMEM((2, 2, 6 * own, lay.lanes), bf16),
                pltpu.VMEM((1, nz), f32),
                pltpu.VMEM((1, nz), f32),
                pltpu.VMEM((plane - 1, nz), f32),
                pltpu.VMEM((near, nz), f32),
                pltpu.VMEM((max(far, 1), nz), f32),
                dma,
                dma((7,)),
                dma((halos,)),
                dma((halos,)),
                dma((2,)),
                dma((2,)),
                *[dma] * 6,
                pltpu.SemaphoreType.REGULAR((8,)),
            ],
            compiler_params=pltpu.CompilerParams(
                collective_id=0, has_side_effects=True
            ),
            name="cell",
        )(fields.reshape(6, nx * ny, nz), macro_strain, material, *consts)
        entries = 3.0 * nx * ny * nz * n["gx"] * n["gy"] * n["gz"]
        block = jax.ShapeDtypeStruct((3 * own, nz), f32)
        residual, tangent, stats = pl.pallas_call(
            functools.partial(finish, entries),
            out_shape=(block, block, jax.ShapeDtypeStruct((2,), f32)),
            in_specs=[vmem, vmem],
            out_specs=(hbm, hbm, hbm),
            scratch_shapes=[pltpu.SMEM((2,), f32), dma((3,))],
            compiler_params=pltpu.CompilerParams(vmem_limit_bytes=24 * 2**20),
            name="finish",
        )(out, totals)
        shape = (3, nx, ny, nz)
        return residual.reshape(shape), tangent.reshape(shape), stats

    in_specs = (P("body", None, "gx", "gy", "gz"), P("body", None), P("body"))
    out_specs = (P("body", "gx", "gy", "gz"), P("body", "gx", "gy", "gz"), P("body"))
    return jax.shard_map(local, mesh=mesh, in_specs=in_specs, out_specs=out_specs, check_vma=False)
```
